32 devices in a mesh: gx: 4 (over y, core), gy: 2 (over x), ta: 4 (over z).
Axes of the slice: x: 2, y: 2, z: 4, core: 2. Of those that a mesh axis runs over, the one named last changes fastest.
Arguments:
- link_x: float32 [2, 3, 3, 16, 16, 256], P(None, None, None, 'gx', 'ta', 'gy'), may hold values from -1 to 1, as said below
- link_t: float32 [2, 3, 3, 16, 16, 256], P(None, None, None, 'gx', 'ta', 'gy'), may hold values from -1 to 1, as said below
Outputs:
- loops: float32 [6, 6, 16, 16], P(None, None, 'gx', 'ta')
The draws below stay inside these ranges and needn't reach their ends.
Inputs may be any that keep to these rules, and one draw needn't show every extreme that they name: `link_x`: every link matrix is special unitary. `link_t`: every link matrix is special unitary.
All inputs are finite; a program needn't handle non-finite values.
Results may differ from the reference program's by a relative error of at most 0.0001.
Values sent between devices are 32-bit elements; how exact they have to be, the bound alone decides.
No kernel may reach another device: no remote copies, remote signals or barrier semaphores. Data moves between devices by JAX's collectives and lax.ppermute only.
A program may use at most 128 MiB of HBM per device.

```python
import jax
import jax.numpy as jnp

RMAX = 6
TMAX = 6
NX = 16
NT = 16
SPECT = 256


def complex_times(left_mat, right_mat):
    real_rows = []
    imag_rows = []
    for i in range(3):
        real_cols = []
        imag_cols = []
        for k in range(3):
            real_sum = left_mat[0][i][0] * right_mat[0][0][k] - left_mat[1][i][0] * right_mat[1][0][k]
            imag_sum = left_mat[0][i][0] * right_mat[1][0][k] + left_mat[1][i][0] * right_mat[0][0][k]
            for j in range(1, 3):
                real_sum = real_sum + left_mat[0][i][j] * right_mat[0][j][k] - left_mat[1][i][j] * right_mat[1][j][k]
                imag_sum = imag_sum + left_mat[0][i][j] * right_mat[1][j][k] + left_mat[1][i][j] * right_mat[0][j][k]
            real_cols.append(real_sum)
            imag_cols.append(imag_sum)
        real_rows.append(real_cols)
        imag_rows.append(imag_cols)
    return [real_rows, imag_rows]


def embed(theta, phi, psi, first, second):
    ones = jnp.ones_like(theta)
    zeros = jnp.zeros_like(theta)
    real_rows = [[ones if i == k else zeros for k in range(3)] for i in range(3)]
    imag_rows = [[zeros for k in range(3)] for i in range(3)]
    cos_t = jnp.cos(theta)
    sin_t = jnp.sin(theta)
    real_rows[first][first] = cos_t * jnp.cos(phi)
    imag_rows[first][first] = cos_t * jnp.sin(phi)
    real_rows[second][second] = cos_t * jnp.cos(phi)
    imag_rows[second][second] = -cos_t * jnp.sin(phi)
    real_rows[first][second] = sin_t * jnp.cos(psi)
    imag_rows[first][second] = sin_t * jnp.sin(psi)
    real_rows[second][first] = -sin_t * jnp.cos(psi)
    imag_rows[second][first] = sin_t * jnp.sin(psi)
    return [real_rows, imag_rows]


def near_identity(key):
    site_shape = (3, NX, NT, SPECT)
    keys = jax.random.split(key, 3)
    theta = jnp.clip(jax.random.normal(keys[0], site_shape, jnp.float32) * 0.35, -1.2, 1.2)
    phi = jnp.clip(jax.random.normal(keys[1], site_shape, jnp.float32) * 0.35, -1.2, 1.2)
    psi = jax.random.uniform(keys[2], site_shape, jnp.float32, -3.14159265, 3.14159265)
    result = embed(theta[0], phi[0], psi[0], 0, 1)
    result = complex_times(result, embed(theta[1], phi[1], psi[1], 1, 2))
    result = complex_times(result, embed(theta[2], phi[2], psi[2], 0, 2))
    real_part = jnp.stack([jnp.stack(row) for row in result[0]])
    imag_part = jnp.stack([jnp.stack(row) for row in result[1]])
    return jnp.stack([real_part, imag_part])


def draw_link_x(key, part):
    return near_identity(jax.random.fold_in(key, 11))


def draw_link_t(key, part):
    return near_identity(jax.random.fold_in(key, 23))


def setup_inputs(seed: int = 0) -> dict:
    splits = jax.random.split(jax.random.key(seed), 3)
    return {
        "link_x": draw_link_x(jax.random.fold_in(splits[2], 71), 0),
        "link_t": draw_link_t(jax.random.fold_in(splits[2], 71), 0),
    }


def times(left_mat, right_mat):
    real_rows = []
    imag_rows = []
    for i in range(3):
        real_cols = []
        imag_cols = []
        for k in range(3):
            real_sum = left_mat[0, i, 0] * right_mat[0, 0, k] - left_mat[1, i, 0] * right_mat[1, 0, k]
            imag_sum = left_mat[0, i, 0] * right_mat[1, 0, k] + left_mat[1, i, 0] * right_mat[0, 0, k]
            for j in range(1, 3):
                real_sum = real_sum + left_mat[0, i, j] * right_mat[0, j, k] - left_mat[1, i, j] * right_mat[1, j, k]
                imag_sum = imag_sum + left_mat[0, i, j] * right_mat[1, j, k] + left_mat[1, i, j] * right_mat[0, j, k]
            real_cols.append(real_sum)
            imag_cols.append(imag_sum)
        real_rows.append(jnp.stack(real_cols))
        imag_rows.append(jnp.stack(imag_cols))
    return jnp.stack([jnp.stack(real_rows), jnp.stack(imag_rows)])


def correlation(upper_half, lower_half):
    return jnp.sum(upper_half * lower_half, axis=(0, 1, 2, 5))


def reference(link_x, link_t):
    temporal = [link_t]
    factor = link_t
    for extent in range(1, TMAX):
        factor = jnp.roll(factor, -1, axis=4)
        temporal.append(times(temporal[-1], factor))
    carried = list(temporal)
    spatial = link_x
    factor_x = link_x
    all_rows = []
    for radius in range(RMAX):
        if radius > 0:
            factor_x = jnp.roll(factor_x, -1, axis=3)
            spatial = times(spatial, factor_x)
        carried = [jnp.roll(field, -1, axis=3) for field in carried]
        shifted = spatial
        row_sums = []
        for extent in range(TMAX):
            shifted = jnp.roll(shifted, -1, axis=4)
            upper_half = times(spatial, carried[extent])
            lower_half = times(temporal[extent], shifted)
            row_sums.append(correlation(upper_half, lower_half))
        all_rows.append(jnp.stack(row_sums))
    return jnp.stack(all_rows) / (3.0 * SPECT)
```

```python
import jax
import jax.numpy as jnp
from jax import lax
from jax.experimental import pallas as pl
from jax.experimental.pallas import tpu as pltpu
from jax.sharding import PartitionSpec as P

RMAX = 6
TMAX = 6


def mul(a, b):
    return a[0] * b[0] - a[1] * b[1], a[0] * b[1] + a[1] * b[0]


def mul_conj(a, b):
    return a[0] * b[0] + a[1] * b[1], a[1] * b[0] - a[0] * b[1]


def add(a, b):
    return a[0] + b[0], a[1] + b[1]


def product(a, b):
    return [
        [add(add(mul(row[0], b[0][k]), mul(row[1], b[1][k])), mul(row[2], b[2][k])) for k in range(3)]
        for row in a
    ]


def product_dagger(a, b):
    return [
        [
            add(add(mul_conj(row[0], b[k][0]), mul_conj(row[1], b[k][1])), mul_conj(row[2], b[k][2]))
            for k in range(3)
        ]
        for row in a
    ]


def completed(a):
    last = []
    for k in range(3):
        i, j = (k + 1) % 3, (k + 2) % 3
        p, q = mul(a[0][i], a[1][j]), mul(a[0][j], a[1][i])
        last.append((p[0] - q[0], q[1] - p[1]))
    return [a[0], a[1], last]


def get(load, rows=2):
    return [[(load((3 * i + j) * 2), load((3 * i + j) * 2 + 1)) for j in range(3)] for i in range(rows)]


def put(store, a):
    for i, row in enumerate(a):
        for j in range(3):
            for k in range(2):
                store((3 * i + j) * 2 + k, row[j][k])


def where(mask, a, b):
    return [[tuple(jnp.where(mask, p, q) for p, q in zip(u, v)) for u, v in zip(r, s)] for r, s in zip(a, b)]


def unit(shape, rows=2):
    one, zero = jnp.ones(shape, jnp.float32), jnp.zeros(shape, jnp.float32)
    return [[(one if i == j else zero, zero) for j in range(3)] for i in range(rows)]


def gauge_kernel(n, x_ref, t_ref, near_ref, far_ref, g_ref, u_ref):
    lanes = x_ref.shape[-1]

    def raw(ref, t, rows):
        part = lambda p, i, j: ref[p * 9 + i * 3 + j, pl.ds(t, n, stride=n), :]
        return [[(part(0, i, j), part(1, i, j)) for j in range(3)] for i in range(rows)]

    g = unit((n, lanes))
    for t in range(n):
        rows = pl.ds(t * n, n)
        put(lambda c, v: g_ref.__setitem__((c, rows), v), completed(g))
        full = raw(x_ref, t, 3)
        put(lambda c, v: u_ref.__setitem__((c, rows), v), product(g, full) if t else full[:2])
        step = raw(t_ref, t, 3)
        g = product(g, step) if t else step[:2]
    put(lambda c, v: near_ref.__setitem__((c, pl.ds(n * n + n, n)), v), g)
    put(
        lambda c, v: near_ref.__setitem__((c, pl.ds(n * n, n)), v),
        get(lambda c: g_ref[c, pl.ds(0, n, stride=n), :]),
    )
    for i in range(0, n * n, 8):
        last = lax.broadcasted_iota(jnp.int32, (8, lanes), 0) % n == n - 1
        after = where(last, unit((8, lanes), 3), get(lambda c: g_ref[c, pl.ds(i + 1, 8), :], 3))
        w = product_dagger(get(lambda c: u_ref[c, pl.ds(i, 8), :]), after)
        put(lambda c, v: near_ref.__setitem__((c, pl.ds(i, 8)), v), w)
    two = 2 * n
    for c in range(12):
        far_ref[pl.ds(c * (two + 2), two), :] = near_ref[c, pl.ds(0, two), :]
        far_ref[pl.ds(c * (two + 2) + two, 2), :] = near_ref[c, pl.ds(n * n, 2), :]


def chain_kernel(n, own_ref, near_ref, far_ref, out_ref, out2_ref, p_ref, q_ref):
    lanes = own_ref.shape[-1]
    times = 2 * n + 2
    size, two = times * (n + 1), 2 * n
    store_w = lambda first, count: lambda c, v: out_ref.__setitem__((pl.ds(c * size + first, count),), v)
    for c in range(12):
        out_ref[pl.ds(c * size, n * n), :] = own_ref[c, pl.ds(0, n * n), :]
        out_ref[pl.ds(c * size + times * n, n), :] = own_ref[c, pl.ds(n * n, n), :]

    def spread(p):
        p = completed(p)
        for k in range(3):
            put(lambda c, v: p_ref.__setitem__((c, pl.ds(k * n, n)), v), p)
        left = get(lambda c: p_ref[c, pl.ds(0, two), :])
        right = get(lambda c: p_ref[c, pl.ds(1, two), :], 3)
        last = lax.broadcasted_iota(jnp.int32, (two, lanes), 0) % n == n - 1
        return left, where(last, unit((two, lanes), 3), right)

    def first_of(p, count):
        return [[tuple(jnp.broadcast_to(e[0:1], (count, lanes)) for e in q) for q in row] for row in p]

    end = pl.ds(n * n + n, n)
    p = get(lambda c: own_ref[c, end, :])
    p_next = get(lambda c: near_ref[c, end, :])
    pp = product(p, completed(p_next))
    left, right = spread(p)
    for i in range(0, n * n, 8):
        w = get(lambda c: near_ref[c, pl.ds(i, 8), :])
        w = product_dagger(product(left, completed(w)), right)
        put(store_w(n * n + i, 8), w)
    g = get(lambda c: near_ref[c, pl.ds(n * n, n), :])
    put(store_w(times * n + n, n), product(first_of(p, n), completed(g)))
    left, right = spread(pp)
    w = get(lambda c: far_ref[pl.ds(c * (two + 2), two), :])
    w = product_dagger(product(left, completed(w)), right)
    put(store_w(2 * n * n, two), w)
    g = get(lambda c: far_ref[pl.ds(c * (two + 2) + two, 2), :])
    put(store_w(times * n + two, 2), product(first_of(pp, 2), completed(g)))
    for c in range(12):
        for first, count in ((0, 8), (8, times - 8)):
            out2_ref[pl.ds(c * two_times(n) + first, count), :] = out_ref[
                pl.ds(c * size + first * n, count, stride=n), :
            ]
            out2_ref[pl.ds(c * two_times(n) + times + first, count), :] = out_ref[
                pl.ds(c * size + times * n + first, count), :
            ]


def two_times(n):
    return 2 * (2 * n + 2)


def loop_kernel(n, own_ref, near_ref, far_ref, out_ref, a_ref, b_ref, c_ref, s_ref):
    lanes = own_ref.shape[-1]
    times = 2 * n + 2
    count = times * n
    size = times * (n + 1)
    pad = 8
    for c in range(12):
        for ref, src in ((a_ref, own_ref), (b_ref, near_ref)):
            for i in range(0, count, 8):
                ref[c, pl.ds(pad + i, 8), :] = src[pl.ds(c * size + i, 8), :]
        for first, m in ((0, 8), (8, times - 8)):
            c_ref[c, pl.ds(n - 1 + first * n, m, stride=n), :] = far_ref[pl.ds(c * 2 * times + first, m), :]
    for ref, g_of in (
        (a_ref, lambda c, f, m: near_ref[pl.ds(c * size + count + f, m), :]),
        (b_ref, lambda c, f, m: far_ref[pl.ds(c * 2 * times + times + f, m), :]),
    ):
        for first, m in ((0, 8), (8, times - 8)):
            rows = pl.ds(pad + n - 1 + first * n, m, stride=n)
            v = get(lambda c: ref[c, rows, :])
            g = completed(get(lambda c: g_of(c, first, m)))
            put(lambda c, e: ref.__setitem__((c, rows), e), product_dagger(v, g))

    x_of = lax.broadcasted_iota(jnp.int32, (8, lanes), 0) % n

    def window(k, i):
        if k == 0:
            return get(lambda c: a_ref[c, pl.ds(pad + i, 8), :])
        if k < n:
            return where(
                x_of < n - k,
                get(lambda c: a_ref[c, pl.ds(pad + i + k, 8), :]),
                get(lambda c: b_ref[c, pl.ds(pad + i + k - n, 8), :]),
            )
        if k == n:
            return get(lambda c: b_ref[c, pl.ds(pad + i, 8), :])
        return where(
            x_of < n - 1,
            get(lambda c: b_ref[c, pl.ds(pad + i + 1, 8), :]),
            get(lambda c: c_ref[c, pl.ds(i, 8), :]),
        )

    for i in range(0, count, 8):
        s = window(0, i)
        for r in range(RMAX):
            if r:
                s = product(s, completed(window(r, i)))
            put(lambda c, v: s_ref.__setitem__((r * 18 + c, pl.ds(i, 8)), v), completed(s))

    lane = lax.broadcasted_iota(jnp.int32, (8, lanes), 1)
    late = lax.broadcasted_iota(jnp.int32, (8, lanes), 0) // n
    half = RMAX // 2
    packed = []
    for r in range(RMAX):
        sums = [[None, None] for _ in range(TMAX)]
        for c in range(18):
            at = {t: s_ref[r * 18 + c, pl.ds(t * n, 8), :] for t in range(times - 1)}
            for u in range(1, TMAX + 1):
                for h in range(2):
                    e = at[2 * h] * at[2 * h + u]
                    sums[u - 1][h] = e if c == 0 else sums[u - 1][h] + e
        for u in range(TMAX):
            for h in range(2):
                total = jnp.sum(sums[u][h], axis=1, keepdims=True)
                base = (r % half) * TMAX * n + u * n + 2 * h
                packed.append((r // half, jnp.where(lane == base + late, total, 0.0)))
    for k in range(2):
        v = sum(e for j, e in packed if j == k)
        out_ref[pl.ds(k * n, n), :] = v[0:n] + v[n : 2 * n]


def call(kernel, outs, scratch, *args):
    whole = pl.BlockSpec(memory_space=pltpu.VMEM)
    return pl.pallas_call(
        kernel,
        out_shape=[jax.ShapeDtypeStruct(s, jnp.float32) for s in outs],
        in_specs=[whole] * len(args),
        out_specs=[whole] * len(outs),
        scratch_shapes=[pltpu.VMEM(s, jnp.float32) for s in scratch],
    )(*args)


def ahead(block, axis, distance):
    count = lax.axis_size(axis)
    return lax.ppermute(block, axis, [((i + distance) % count, i) for i in range(count)])


def local(link_x, link_t):
    n, lanes = link_x.shape[3], link_x.shape[5]
    if (n, link_x.shape[4], lanes) != (4, 4, 128):
        return plain(link_x, link_t)
    times = 2 * n + 2
    flat = (18, n * n, lanes)
    near, far = call(
        lambda *refs: gauge_kernel(n, *refs),
        [(12, n * n + 2 * n, lanes), (12 * (2 * n + 2), lanes)],
        [(18, n * n + 8, lanes), (12, n * n, lanes)],
        link_x.reshape(flat),
        link_t.reshape(flat),
    )
    near_t, far_t = ahead(near, "ta", 1), ahead(far, "ta", 2)
    own, edge = call(
        lambda *refs: chain_kernel(n, *refs),
        [(12 * times * (n + 1), lanes), (12 * 2 * times, lanes)],
        [(18, 3 * n, lanes), (8, lanes)],
        near,
        near_t,
        far_t,
    )
    own_x, edge_x = ahead(own, "gx", 1), ahead(edge, "gx", 2)
    rows = times * n + 16
    (packed,) = call(
        lambda *refs: loop_kernel(n, *refs),
        [(8, lanes)],
        [(12, rows, lanes), (12, rows, lanes), (12, times * n, lanes), (RMAX * 18, times * n, lanes)],
        own,
        own_x,
        edge_x,
    )
    count = lax.axis_size("gy")
    if count == 2:
        packed = packed + ahead(packed, "gy", 1)
    else:
        packed = lax.psum(packed, "gy")
    packed = packed / (3.0 * (lanes * count))
    half = RMAX // 2
    packed = packed[:, : half * TMAX * n].reshape(2, n, half, TMAX, n)
    return packed.transpose(0, 2, 3, 1, 4).reshape(RMAX, TMAX, n, n)


def shifted_2(block, axis, distance):
    devices = range(lax.axis_size(axis))
    route = [((i - distance) % len(devices), i) for i in devices]
    return lax.ppermute(block, axis, route)


def plain_times(left_mat, right_mat):
    real_rows = []
    imag_rows = []
    for i in range(3):
        real_cols = []
        imag_cols = []
        for k in range(3):
            real_sum = (
                left_mat[0, i, 0] * right_mat[0, 0, k] - left_mat[1, i, 0] * right_mat[1, 0, k]
            )
            imag_sum = (
                left_mat[0, i, 0] * right_mat[1, 0, k] + left_mat[1, i, 0] * right_mat[0, 0, k]
            )
            for j in range(1, 3):
                real_sum = (
                    real_sum
                    + left_mat[0, i, j] * right_mat[0, j, k]
                    - left_mat[1, i, j] * right_mat[1, j, k]
                )
                imag_sum = (
                    imag_sum
                    + left_mat[0, i, j] * right_mat[1, j, k]
                    + left_mat[1, i, j] * right_mat[0, j, k]
                )
            real_cols.append(real_sum)
            imag_cols.append(imag_sum)
        real_rows.append(jnp.stack(real_cols))
        imag_rows.append(jnp.stack(imag_cols))
    return jnp.stack([jnp.stack(real_rows), jnp.stack(imag_rows)])


def correlation(upper_half, lower_half):
    return jnp.sum(upper_half * lower_half, axis=(0, 1, 2, 5))


def next_x(field, along_dim):
    edge_cells = shifted_2(lax.slice_in_dim(field, 0, 1, axis=along_dim), "gx", -1)
    inner = lax.slice_in_dim(field, 1, field.shape[along_dim], axis=along_dim)
    return jnp.concatenate([inner, edge_cells], axis=along_dim)


def next_t(field):
    edge_cells = shifted_2(lax.slice_in_dim(field, 0, 1, axis=4), "ta", -1)
    inner = lax.slice_in_dim(field, 1, field.shape[4], axis=4)
    return jnp.concatenate([inner, edge_cells], axis=4)


def plain(link_x, link_t):
    all_rows = []
    temporal = [link_t]
    factor = link_t
    for extent in range(1, TMAX):
        factor = next_t(factor)
        temporal.append(plain_times(temporal[-1], factor))
    carried = jnp.stack(temporal)
    spatial = link_x
    factor_x = link_x
    for radius in range(RMAX):
        if radius > 0:
            factor_x = next_x(factor_x, 3)
            spatial = plain_times(spatial, factor_x)
        carried = next_x(carried, 4)
        shifted = spatial
        row_sums = []
        for extent in range(TMAX):
            shifted = next_t(shifted)
            upper_half = plain_times(spatial, carried[extent])
            lower_half = plain_times(temporal[extent], shifted)
            row_sums.append(correlation(upper_half, lower_half))
        all_rows.append(jnp.stack(row_sums))
    local_sums = jnp.stack(all_rows)
    totals = lax.psum(local_sums, "gy")
    return totals / (3.0 * (link_x.shape[5] * lax.axis_size("gy")))


def solution(mesh):
    return jax.shard_map(
        local,
        mesh=mesh,
        in_specs=(P(None, None, None, "gx", "ta", "gy"), P(None, None, None, "gx", "ta", "gy")),
        out_specs=P(None, None, "gx", "ta"),
        check_vma=False,
    )
```

```python
import jax
import jax.numpy as jnp
from jax import lax
from jax.experimental import pallas as pl
from jax.experimental.pallas import tpu as pltpu
from jax.sharding import PartitionSpec as P


RMAX = 6
TMAX = 6


def mul(a, b):
    return a[0] * b[0] - a[1] * b[1], a[0] * b[1] + a[1] * b[0]


def mul_conj(a, b):
    return a[0] * b[0] + a[1] * b[1], a[1] * b[0] - a[0] * b[1]


def add(a, b):
    return a[0] + b[0], a[1] + b[1]


def product(a, b):
    return [
        [add(add(mul(row[0], b[0][k]), mul(row[1], b[1][k])), mul(row[2], b[2][k])) for k in range(3)]
        for row in a
    ]


def product_dagger(a, b):
    return [
        [
            add(add(mul_conj(row[0], b[k][0]), mul_conj(row[1], b[k][1])), mul_conj(row[2], b[k][2]))
            for k in range(3)
        ]
        for row in a
    ]


def completed(a):
    last = []
    for k in range(3):
        i, j = (k + 1) % 3, (k + 2) % 3
        p, q = mul(a[0][i], a[1][j]), mul(a[0][j], a[1][i])
        last.append((p[0] - q[0], q[1] - p[1]))
    return [a[0], a[1], last]


def get(load, rows=2):
    return [[(load((3 * i + j) * 2), load((3 * i + j) * 2 + 1)) for j in range(3)] for i in range(rows)]


def put(store, a):
    for i, row in enumerate(a):
        for j in range(3):
            for k in range(2):
                store((3 * i + j) * 2 + k, row[j][k])


def where(mask, a, b):
    return [[tuple(jnp.where(mask, p, q) for p, q in zip(u, v)) for u, v in zip(r, s)] for r, s in zip(a, b)]


def unit(shape, rows=2):
    one, zero = jnp.ones(shape, jnp.float32), jnp.zeros(shape, jnp.float32)
    return [[(one if i == j else zero, zero) for j in range(3)] for i in range(rows)]


def gauge_kernel(n, links_ref, near_ref, far_ref, edge_ref, g_ref, u_ref):
    lanes = links_ref.shape[-1]
    x_ref, t_ref = links_ref.at[0], links_ref.at[1]

    def raw(ref, t, rows):
        part = lambda p, i, j: ref[p * 9 + i * 3 + j, pl.ds(t, n, stride=n), :]
        return [[(part(0, i, j), part(1, i, j)) for j in range(3)] for i in range(rows)]

    g = unit((n, lanes))
    for t in range(n):
        rows = pl.ds(t * n, n)
        put(lambda c, v: g_ref.__setitem__((c, rows), v), completed(g))
        full = raw(x_ref, t, 3)
        put(lambda c, v: u_ref.__setitem__((c, rows), v), product(g, full) if t else full[:2])
        step = raw(t_ref, t, 3)
        g = product(g, step) if t else step[:2]
    put(lambda c, v: near_ref.__setitem__((c, pl.ds(n * n + n, n)), v), g)
    put(
        lambda c, v: near_ref.__setitem__((c, pl.ds(n * n, n)), v),
        get(lambda c: g_ref[c, pl.ds(0, n, stride=n), :]),
    )
    for i in range(0, n * n, 8):
        last = lax.broadcasted_iota(jnp.int32, (8, lanes), 0) % n == n - 1
        after = where(last, unit((8, lanes), 3), get(lambda c: g_ref[c, pl.ds(i + 1, 8), :], 3))
        w = product_dagger(get(lambda c: u_ref[c, pl.ds(i, 8), :]), after)
        put(lambda c, v: near_ref.__setitem__((c, pl.ds(i, 8)), v), w)
    two = 2 * n
    for c in range(12):
        far_ref[pl.ds(c * (two + 2), two), :] = near_ref[c, pl.ds(0, two), :]
        far_ref[pl.ds(c * (two + 2) + two, 2), :] = near_ref[c, pl.ds(n * n, 2), :]
        edge_ref[pl.ds(c * two, n), :] = near_ref[c, pl.ds(0, n, stride=n), :]
        edge_ref[pl.ds(c * two + n, n), :] = near_ref[c, pl.ds(n * n, n), :]


def chain_kernel(n, own_ref, near_ref, far_ref, out_ref, edge_ref, p_ref):
    lanes = own_ref.shape[-1]
    late, two = n + 2, 2 * n
    size = late * (n + 1)
    store_w = lambda first, count: lambda c, v: out_ref.__setitem__((pl.ds(c * size + first, count),), v)

    def spread(p):
        p = completed(p)
        for k in range(3):
            put(lambda c, v: p_ref.__setitem__((c, pl.ds(k * n, n)), v), p)
        left = get(lambda c: p_ref[c, pl.ds(0, two), :])
        right = get(lambda c: p_ref[c, pl.ds(1, two), :], 3)
        last = lax.broadcasted_iota(jnp.int32, (two, lanes), 0) % n == n - 1
        return left, where(last, unit((two, lanes), 3), right)

    def first_of(p, count):
        return [[tuple(jnp.broadcast_to(e[0:1], (count, lanes)) for e in q) for q in row] for row in p]

    end = pl.ds(n * n + n, n)
    p = get(lambda c: own_ref[c, end, :])
    p_next = get(lambda c: near_ref[c, end, :])
    pp = product(p, completed(p_next))
    left, right = spread(p)
    for i in range(0, n * n, 8):
        w = get(lambda c: near_ref[c, pl.ds(i, 8), :])
        w = product_dagger(product(left, completed(w)), right)
        put(store_w(i, 8), w)
    g = get(lambda c: near_ref[c, pl.ds(n * n, n), :])
    put(store_w(late * n, n), product(first_of(p, n), completed(g)))
    left, right = spread(pp)
    w = get(lambda c: far_ref[pl.ds(c * (two + 2), two), :])
    w = product_dagger(product(left, completed(w)), right)
    put(store_w(n * n, two), w)
    g = get(lambda c: far_ref[pl.ds(c * (two + 2) + two, 2), :])
    put(store_w(late * n + n, 2), product(first_of(pp, 2), completed(g)))
    for c in range(12):
        edge_ref[pl.ds(c * 2 * late, late), :] = out_ref[pl.ds(c * size, late, stride=n), :]
        edge_ref[pl.ds(c * 2 * late + late, late), :] = out_ref[pl.ds(c * size + late * n, late), :]


def loop_kernel(
    n, own_ref, own2_ref, near_ref, near2_ref, far_ref, far2_ref, out_ref, a_ref, b_ref, c_ref, s_ref
):
    lanes = own_ref.shape[-1]
    late, early = n + 2, n * n
    times = n + late
    count = times * n
    size = late * (n + 1)
    pad = 8
    for c in range(12):
        for ref, src, src2 in ((a_ref, own_ref, own2_ref), (b_ref, near_ref, near2_ref)):
            for i in range(0, early, 8):
                ref[c, pl.ds(pad + i, 8), :] = src[c, pl.ds(i, 8), :]
            for i in range(0, late * n, 8):
                ref[c, pl.ds(pad + early + i, 8), :] = src2[pl.ds(c * size + i, 8), :]
        c_ref[c, pl.ds(n - 1, n, stride=n), :] = far_ref[pl.ds(c * 2 * n, n), :]
        c_ref[c, pl.ds(early + n - 1, late, stride=n), :] = far2_ref[pl.ds(c * 2 * late, late), :]
    for ref, g_of in (
        (
            a_ref,
            (
                lambda c: near_ref[c, pl.ds(early, n), :],
                lambda c: near2_ref[pl.ds(c * size + late * n, late), :],
            ),
        ),
        (
            b_ref,
            (
                lambda c: far_ref[pl.ds(c * 2 * n + n, n), :],
                lambda c: far2_ref[pl.ds(c * 2 * late + late, late), :],
            ),
        ),
    ):
        for first, m, g in ((0, n, g_of[0]), (n, late, g_of[1])):
            rows = pl.ds(pad + n - 1 + first * n, m, stride=n)
            v = product_dagger(get(lambda c: ref[c, rows, :]), completed(get(g)))
            put(lambda c, e: ref.__setitem__((c, rows), e), v)

    x_of = lax.broadcasted_iota(jnp.int32, (8, lanes), 0) % n

    def window(k, i):
        if k == 0:
            return get(lambda c: a_ref[c, pl.ds(pad + i, 8), :])
        if k < n:
            return where(
                x_of < n - k,
                get(lambda c: a_ref[c, pl.ds(pad + i + k, 8), :]),
                get(lambda c: b_ref[c, pl.ds(pad + i + k - n, 8), :]),
            )
        if k == n:
            return get(lambda c: b_ref[c, pl.ds(pad + i, 8), :])
        return where(
            x_of < n - 1,
            get(lambda c: b_ref[c, pl.ds(pad + i + 1, 8), :]),
            get(lambda c: c_ref[c, pl.ds(i, 8), :]),
        )

    for i in range(0, count, 8):
        s = window(0, i)
        for r in range(RMAX):
            if r:
                s = product(s, completed(window(r, i)))
            put(lambda c, v: s_ref.__setitem__((r * 18 + c, pl.ds(i, 8)), v), completed(s))

    lane = lax.broadcasted_iota(jnp.int32, (8, lanes), 1)
    packed = [jnp.zeros((8, lanes), jnp.float32)] * 2
    for r in range(RMAX):
        sums = [[None, None] for _ in range(TMAX)]
        for c in range(18):
            at = {t: s_ref[r * 18 + c, pl.ds(t * n, 8), :] for t in range(times - 1)}
            for u in range(1, TMAX + 1):
                for h in range(2):
                    e = at[2 * h] * at[2 * h + u]
                    sums[u - 1][h] = e if c == 0 else sums[u - 1][h] + e
        for u in range(TMAX):
            for h in range(2):
                total = jnp.sum(sums[u][h], axis=1, keepdims=True)
                packed[h] = jnp.where(lane == r * TMAX + u, total, packed[h])
    for h in range(2):
        out_ref[pl.ds(8 * h, 8), :] = packed[h]


def last_kernel(n, scale, own_ref, other_ref, out_ref, v_ref):
    lanes = own_ref.shape[-1]
    total = (own_ref[...] + other_ref[...]) * scale
    for r in range(RMAX):
        v_ref[r] = pltpu.roll(total, lanes - r * TMAX, 1) if r else total
        for x in range(n):
            out_ref[r, x] = v_ref[r, pl.ds(x, n, stride=n), :][:, :TMAX]


def call(kernel, outs, scratch, *args, space=pltpu.VMEM):
    return pl.pallas_call(
        kernel,
        out_shape=[jax.ShapeDtypeStruct(s, jnp.float32) for s in outs],
        in_specs=[pl.BlockSpec(memory_space=space)] * len(args),
        out_specs=[pl.BlockSpec(memory_space=pltpu.VMEM)] * len(outs),
        scratch_shapes=[pltpu.VMEM(s, jnp.float32) if isinstance(s, tuple) else s for s in scratch],
        compiler_params=pltpu.CompilerParams(vmem_limit_bytes=8 * 2**20),
    )(*args)


def ahead(block, axis, distance):
    count = lax.axis_size(axis)
    return lax.ppermute(block, axis, [((i + distance) % count, i) for i in range(count)])


def local(link_x, link_t):
    n, lanes = link_x.shape[3], link_x.shape[5]
    if (n, link_x.shape[4], lanes) != (4, 4, 128):
        return plain(link_x, link_t)
    late = n + 2
    times = n + late
    flat = (18, n * n, lanes)
    own, far, edge = call(
        lambda *refs: gauge_kernel(n, *refs),
        [(12, n * n + 2 * n, lanes), (12 * (2 * n + 2), lanes), (12 * 2 * n, lanes)],
        [(18, n * n + 8, lanes), (12, n * n, lanes)],
        jnp.stack([link_x.reshape(flat), link_t.reshape(flat)]),
    )
    near_t, far_t = ahead(own, "ta", 1), ahead(far, "ta", 2)
    near_x, edge_x = ahead(own, "gx", 1), ahead(edge, "gx", 2)
    own2, edge2 = call(
        lambda *refs: chain_kernel(n, *refs),
        [(12 * late * (n + 1), lanes), (12 * 2 * late, lanes)],
        [(18, 3 * n, lanes)],
        own,
        near_t,
        far_t,
    )
    near2_x, edge2_x = ahead(own2, "gx", 1), ahead(edge2, "gx", 2)
    rows = times * n + 16
    (packed,) = call(
        lambda *refs: loop_kernel(n, *refs),
        [(16, lanes)],
        [(12, rows, lanes), (12, rows, lanes), (12, times * n, lanes), (RMAX * 18, times * n, lanes)],
        own,
        own2,
        near_x,
        near2_x,
        edge_x,
        edge2_x,
    )
    count = lax.axis_size("gy")
    other = ahead(packed, "gy", 1) if count == 2 else lax.psum(packed, "gy") - packed
    scale = 1.0 / (3.0 * (lanes * count))
    (out,) = call(
        lambda *refs: last_kernel(n, scale, *refs),
        [(RMAX, n, n, TMAX)],
        [(RMAX, 4 * n, lanes)],
        packed,
        other,
    )
    return out.transpose(0, 3, 1, 2)


def shifted_2(block, axis, distance):
    devices = range(lax.axis_size(axis))
    route = [((i - distance) % len(devices), i) for i in devices]
    return lax.ppermute(block, axis, route)


def plain_times(left_mat, right_mat):
    real_rows = []
    imag_rows = []
    for i in range(3):
        real_cols = []
        imag_cols = []
        for k in range(3):
            real_sum = (
                left_mat[0, i, 0] * right_mat[0, 0, k] - left_mat[1, i, 0] * right_mat[1, 0, k]
            )
            imag_sum = (
                left_mat[0, i, 0] * right_mat[1, 0, k] + left_mat[1, i, 0] * right_mat[0, 0, k]
            )
            for j in range(1, 3):
                real_sum = (
                    real_sum
                    + left_mat[0, i, j] * right_mat[0, j, k]
                    - left_mat[1, i, j] * right_mat[1, j, k]
                )
                imag_sum = (
                    imag_sum
                    + left_mat[0, i, j] * right_mat[1, j, k]
                    + left_mat[1, i, j] * right_mat[0, j, k]
                )
            real_cols.append(real_sum)
            imag_cols.append(imag_sum)
        real_rows.append(jnp.stack(real_cols))
        imag_rows.append(jnp.stack(imag_cols))
    return jnp.stack([jnp.stack(real_rows), jnp.stack(imag_rows)])


def correlation(upper_half, lower_half):
    return jnp.sum(upper_half * lower_half, axis=(0, 1, 2, 5))


def next_x(field, along_dim):
    edge_cells = shifted_2(lax.slice_in_dim(field, 0, 1, axis=along_dim), "gx", -1)
    inner = lax.slice_in_dim(field, 1, field.shape[along_dim], axis=along_dim)
    return jnp.concatenate([inner, edge_cells], axis=along_dim)


def next_t(field):
    edge_cells = shifted_2(lax.slice_in_dim(field, 0, 1, axis=4), "ta", -1)
    inner = lax.slice_in_dim(field, 1, field.shape[4], axis=4)
    return jnp.concatenate([inner, edge_cells], axis=4)


def plain(link_x, link_t):
    all_rows = []
    temporal = [link_t]
    factor = link_t
    for _ in range(1, TMAX):
        factor = next_t(factor)
        temporal.append(plain_times(temporal[-1], factor))
    carried = jnp.stack(temporal)
    spatial = link_x
    factor_x = link_x
    for radius in range(RMAX):
        if radius > 0:
            factor_x = next_x(factor_x, 3)
            spatial = plain_times(spatial, factor_x)
        carried = next_x(carried, 4)
        shifted = spatial
        row_sums = []
        for extent in range(TMAX):
            shifted = next_t(shifted)
            upper_half = plain_times(spatial, carried[extent])
            lower_half = plain_times(temporal[extent], shifted)
            row_sums.append(correlation(upper_half, lower_half))
        all_rows.append(jnp.stack(row_sums))
    local_sums = jnp.stack(all_rows)
    totals = lax.psum(local_sums, "gy")
    return totals / (3.0 * (link_x.shape[5] * lax.axis_size("gy")))


def solution(mesh):
    return jax.shard_map(
        local,
        mesh=mesh,
        in_specs=(P(None, None, None, "gx", "ta", "gy"), P(None, None, None, "gx", "ta", "gy")),
        out_specs=P(None, None, "gx", "ta"),
        check_vma=False,
    )
```

```python
import jax
import jax.numpy as jnp
from jax import lax
from jax.experimental import pallas as pl
from jax.experimental.pallas import tpu as pltpu
from jax.sharding import PartitionSpec as P


RMAX = 6
TMAX = 6


def mul(a, b):
    return a[0] * b[0] - a[1] * b[1], a[0] * b[1] + a[1] * b[0]


def mul_conj(a, b):
    return a[0] * b[0] + a[1] * b[1], a[1] * b[0] - a[0] * b[1]


def add(a, b):
    return a[0] + b[0], a[1] + b[1]


def product(a, b):
    return [
        [add(add(mul(row[0], b[0][k]), mul(row[1], b[1][k])), mul(row[2], b[2][k])) for k in range(3)]
        for row in a
    ]


def product_dagger(a, b):
    return [
        [
            add(add(mul_conj(row[0], b[k][0]), mul_conj(row[1], b[k][1])), mul_conj(row[2], b[k][2]))
            for k in range(3)
        ]
        for row in a
    ]


def completed(a):
    last = []
    for k in range(3):
        i, j = (k + 1) % 3, (k + 2) % 3
        p, q = mul(a[0][i], a[1][j]), mul(a[0][j], a[1][i])
        last.append((p[0] - q[0], q[1] - p[1]))
    return [a[0], a[1], last]


def get(load, rows=2):
    return [[(load((3 * i + j) * 2), load((3 * i + j) * 2 + 1)) for j in range(3)] for i in range(rows)]


def put(store, a):
    for i, row in enumerate(a):
        for j in range(3):
            for k in range(2):
                store((3 * i + j) * 2 + k, row[j][k])


def where(mask, a, b):
    return [[tuple(jnp.where(mask, p, q) for p, q in zip(u, v)) for u, v in zip(r, s)] for r, s in zip(a, b)]


def unit(shape, rows=2):
    one, zero = jnp.ones(shape, jnp.float32), jnp.zeros(shape, jnp.float32)
    return [[(one if i == j else zero, zero) for j in range(3)] for i in range(rows)]


def pivots(a):
    size = [v[0] * v[0] + v[1] * v[1] for v in a]
    first = jnp.logical_and(size[0] >= size[1], size[0] >= size[2])
    last = jnp.logical_and(jnp.logical_not(first), size[2] > size[1])
    return size, first, last


def pick(mask, p, q):
    return tuple(jnp.where(mask, u, v) for u, v in zip(p, q))


def sent(m):
    a, b = m[0], m[1]
    _, first, last = pivots(a)
    return [e for v in (*a, pick(first, b[1], b[0]), pick(last, b[1], b[2])) for e in v]


def received(load):
    v = [(load(2 * k), load(2 * k + 1)) for k in range(5)]
    a, e, f = v[:3], v[3], v[4]
    size, first, last = pivots(a)
    p, q = pick(first, a[1], a[0]), pick(last, a[1], a[2])
    top = pick(first, a[0], pick(last, a[2], a[1]))
    scale = -1.0 / jnp.maximum(jnp.maximum(size[0], size[1]), size[2])
    g = mul(add(mul_conj(e, p), mul_conj(f, q)), top)
    g = (g[0] * scale, g[1] * scale)
    return [a, [pick(first, g, e), pick(first, e, pick(last, f, g)), pick(last, g, f)]]


def send(store, m):
    for k, e in enumerate(sent(m)):
        store(k, e)


def at_rows(ref, rows_of_value):
    def store(k, v):
        ref[rows_of_value(k)] = v

    return store


def flat_rows(ref, size, first, count, stride=None):
    rows = lambda k: pl.ds(k * size + first, count, stride=stride)
    return lambda k: ref[rows(k), :], at_rows(ref, rows)


def rows_of(ref, first, count, stride=None, offset=0):
    rows = pl.ds(first, count, stride=stride)
    return lambda k: ref[offset + k, rows, :], at_rows(ref, lambda k: (offset + k, rows))


def gauge_kernel(n, links_ref, own_ref, near_ref, far_ref, edge_ref, g_ref, u_ref):
    lanes = links_ref.shape[-1]
    block = n * n
    near, far, edge = block + 2 * n - 1, 2 * n + 1, 2 * n - 1

    def raw(field, t, rows):
        part = lambda p, i, j: links_ref[field, p * 9 + i * 3 + j, pl.ds(t, n, stride=n), :]
        return [[(part(0, i, j), part(1, i, j)) for j in range(3)] for i in range(rows)]

    g = unit((n, lanes))
    for t in range(n):
        put(rows_of(g_ref, t * n, n)[1], completed(g))
        full = raw(0, t, 3)
        put(rows_of(u_ref, t * n, n)[1], product(g, full) if t else full[:2])
        step = raw(1, t, 3)
        g = product(g, step) if t else step[:2]
    put(rows_of(own_ref, block + n, n)[1], g)
    send(flat_rows(near_ref, near, block, n)[1], g)
    g = get(rows_of(g_ref, 0, n, n)[0])
    put(rows_of(own_ref, block, n)[1], g)
    g = [[tuple(e[1:] for e in v) for v in row] for row in g]
    send(flat_rows(near_ref, near, block + n, n - 1)[1], g)
    last = lax.broadcasted_iota(jnp.int32, (8, lanes), 0) % n == n - 1
    for i in range(0, block, 8):
        after = where(last, unit((8, lanes), 3), get(rows_of(g_ref, i + 1, 8)[0], 3))
        w = product_dagger(get(rows_of(u_ref, i, 8)[0]), after)
        put(rows_of(own_ref, i, 8)[1], w)
        send(flat_rows(near_ref, near, i, 8)[1], w)
    for k in range(10):
        far_ref[pl.ds(k * far, 2 * n), :] = near_ref[pl.ds(k * near, 2 * n), :]
        far_ref[pl.ds(k * far + 2 * n, 1), :] = near_ref[pl.ds(k * near + block + n, 1), :]
        edge_ref[pl.ds(k * edge, n), :] = near_ref[pl.ds(k * near, n, stride=n), :]
        edge_ref[pl.ds(k * edge + n, n - 1), :] = near_ref[pl.ds(k * near + block + n, n - 1), :]


def chain_kernel(n, own_ref, near_ref, far_ref, out_ref, late_ref, edge_ref, p_ref):
    lanes = own_ref.shape[-1]
    late, two, block = n + 2, 2 * n, n * n
    size = late * (n + 1)
    near, far = block + 2 * n - 1, 2 * n + 1

    def keep(first, count, m):
        put(flat_rows(out_ref, size, first, count)[1], m)
        send(flat_rows(late_ref, size, first, count)[1], m)

    def spread(p):
        p = completed(p)
        for k in range(3):
            put(rows_of(p_ref, k * n, n)[1], p)
        last = lax.broadcasted_iota(jnp.int32, (two, lanes), 0) % n == n - 1
        right = where(last, unit((two, lanes), 3), get(rows_of(p_ref, 1, two)[0], 3))
        return get(rows_of(p_ref, 0, two)[0]), right

    def first_of(p, count):
        return [[tuple(jnp.broadcast_to(e[0:1], (count, lanes)) for e in q) for q in row] for row in p]

    p = get(rows_of(own_ref, block + n, n)[0])
    p_next = received(flat_rows(near_ref, near, block, n)[0])
    pp = product(p, completed(p_next))
    left, right = spread(p)
    for i in range(0, block, 8):
        w = received(flat_rows(near_ref, near, i, 8)[0])
        keep(i, 8, product_dagger(product(left, completed(w)), right))
    keep(late * n, 1, first_of(p, 1))
    g = received(flat_rows(near_ref, near, block + n, n - 1)[0])
    keep(late * n + 1, n - 1, product(first_of(p, n - 1), completed(g)))
    left, right = spread(pp)
    w = received(flat_rows(far_ref, far, 0, two)[0])
    keep(block, two, product_dagger(product(left, completed(w)), right))
    keep(late * n + n, 1, first_of(pp, 1))
    g = received(flat_rows(far_ref, far, two, 1)[0])
    keep(late * n + n + 1, 1, product(first_of(pp, 1), completed(g)))
    for k in range(10):
        edge_ref[pl.ds(k * 2 * late, late), :] = late_ref[pl.ds(k * size, late, stride=n), :]
        edge_ref[pl.ds(k * 2 * late + late, late), :] = late_ref[pl.ds(k * size + late * n, late), :]


PAD = 8


def transports(n, times, a_ref, b_ref, c_ref, closing, store):
    lanes = a_ref.shape[-1]
    for ref, g in zip((a_ref, b_ref), closing):
        load, keep = rows_of(ref, PAD + n - 1, times, n)
        put(keep, product_dagger(get(load), completed(g)))
    x_of = lax.broadcasted_iota(jnp.int32, (8, lanes), 0) % n

    def window(k, i):
        own = lambda shift: get(rows_of(a_ref, PAD + i + shift, 8)[0])
        after = lambda shift: get(rows_of(b_ref, PAD + i + shift, 8)[0])
        if k == 0:
            return own(0)
        if k < n:
            return where(x_of < n - k, own(k), after(k - n))
        if k == n:
            return after(0)
        return where(x_of < n - 1, after(1), get(rows_of(c_ref, i, 8)[0]))

    for i in range(0, times * n, 8):
        s = window(0, i)
        for r in range(RMAX):
            if r:
                s = product(s, completed(window(r, i)))
            put(lambda c, v: store(r * 18 + c, i, v), completed(s))


def paired(pairs, at):
    sums = [None] * len(pairs)
    for c in range(18):
        for k, (p, q) in enumerate(pairs):
            e = at(c, p) * at(c, q)
            sums[k] = e if c == 0 else sums[k] + e
    return [jnp.sum(v, axis=1, keepdims=True) for v in sums]


def early_kernel(n, own_ref, near_ref, far_ref, s_ref, out_ref, a_ref, b_ref, c_ref, g_ref):
    lanes = own_ref.shape[-1]
    block = n * n
    near, edge = block + 2 * n - 1, 2 * n - 1
    for i in range(0, block, 8):
        put(rows_of(a_ref, PAD + i, 8)[1], get(rows_of(own_ref, i, 8)[0]))
        put(rows_of(b_ref, PAD + i, 8)[1], received(flat_rows(near_ref, near, i, 8)[0]))
    put(rows_of(c_ref, n - 1, n, n)[1], received(flat_rows(far_ref, edge, 0, n)[0]))
    closing = []
    for k, load in enumerate((flat_rows(near_ref, near, block + n, n - 1), flat_rows(far_ref, edge, n, n - 1))):
        put(rows_of(g_ref, 0, 1, offset=12 * k)[1], unit((1, lanes)))
        put(rows_of(g_ref, 1, n - 1, offset=12 * k)[1], received(load[0]))
        closing.append(get(rows_of(g_ref, 0, n, offset=12 * k)[0]))

    def store(c, i, v):
        s_ref[c, pl.ds(i, 8), :] = v

    transports(n, n, a_ref, b_ref, c_ref, closing, store)
    lane = lax.broadcasted_iota(jnp.int32, (8, lanes), 1)
    packed = jnp.zeros((8, lanes), jnp.float32)
    for r in range(RMAX):
        at = lambda c, t: s_ref[r * 18 + c, pl.ds(t * n, 8), :]
        for u, total in enumerate(paired([(0, 1), (0, 2)], at)):
            packed = jnp.where(lane == r * TMAX + u, total, packed)
    out_ref[...] = packed


def late_kernel(n, own_ref, near_ref, far_ref, early_ref, packed_ref, out_ref, a_ref, b_ref, c_ref, s_ref):
    lanes = own_ref.shape[-1]
    late = n + 2
    size = late * (n + 1)
    for i in range(0, late * n, 8):
        put(rows_of(a_ref, PAD + i, 8)[1], get(flat_rows(own_ref, size, i, 8)[0]))
        put(rows_of(b_ref, PAD + i, 8)[1], received(flat_rows(near_ref, size, i, 8)[0]))
    put(rows_of(c_ref, n - 1, late, n)[1], received(flat_rows(far_ref, 2 * late, 0, late)[0]))
    closing = [
        received(flat_rows(near_ref, size, late * n, late)[0]),
        received(flat_rows(far_ref, 2 * late, late, late)[0]),
    ]

    def store(c, i, v):
        s_ref[c, pl.ds(n + i, 8), :] = v

    transports(n, late, a_ref, b_ref, c_ref, closing, store)
    for c in range(RMAX * 18):
        s_ref[c, pl.ds(0, n), :] = early_ref[c, pl.ds(n * n - n, n), :]
    lane = lax.broadcasted_iota(jnp.int32, (8, lanes), 1)
    packed = [packed_ref[...], jnp.zeros((8, lanes), jnp.float32)]
    places = [(h, u) for u in range(1, TMAX + 1) for h in range(2) if (h, u) not in ((0, 1), (0, 2))]
    for r in range(RMAX):

        def at(c, t):
            if t < n - 1:
                return early_ref[r * 18 + c, pl.ds(t * n, 8), :]
            return s_ref[r * 18 + c, pl.ds((t - n + 1) * n, 8), :]

        for (h, u), total in zip(places, paired([(2 * h, 2 * h + u) for h, u in places], at)):
            packed[h] = jnp.where(lane == r * TMAX + u - 1, total, packed[h])
    for h in range(2):
        out_ref[pl.ds(8 * h, 8), :] = packed[h]


def last_kernel(n, scale, own_ref, other_ref, out_ref, v_ref):
    lanes = own_ref.shape[-1]
    total = (own_ref[...] + other_ref[...]) * scale
    for r in range(RMAX):
        v_ref[r] = pltpu.roll(total, lanes - r * TMAX, 1) if r else total
        for x in range(n):
            out_ref[r, x] = v_ref[r, pl.ds(x, n, stride=n), :][:, :TMAX]


def call(kernel, outs, scratch, *args, space=pltpu.VMEM):
    return pl.pallas_call(
        kernel,
        out_shape=[jax.ShapeDtypeStruct(s, jnp.float32) for s in outs],
        in_specs=[pl.BlockSpec(memory_space=space)] * len(args),
        out_specs=[pl.BlockSpec(memory_space=pltpu.VMEM)] * len(outs),
        scratch_shapes=[pltpu.VMEM(s, jnp.float32) if isinstance(s, tuple) else s for s in scratch],
        compiler_params=pltpu.CompilerParams(vmem_limit_bytes=8 * 2**20),
    )(*args)


def ahead(block, axis, distance):
    count = lax.axis_size(axis)
    return lax.ppermute(block, axis, [((i + distance) % count, i) for i in range(count)])


def local(link_x, link_t):
    n, lanes = link_x.shape[3], link_x.shape[5]
    if (n, link_x.shape[4], lanes) != (4, 4, 128):
        return plain(link_x, link_t)
    late, block = n + 2, n * n
    size, two = late * (n + 1), 2 * n
    flat = (18, block, lanes)
    own, near, far, edge = call(
        lambda *refs: gauge_kernel(n, *refs),
        [(12, block + two, lanes)] + [(10 * rows, lanes) for rows in (block + two - 1, two + 1, two - 1)],
        [(18, block + 8, lanes), (12, block, lanes)],
        jnp.stack([link_x.reshape(flat), link_t.reshape(flat)]),
    )
    near_t, far_t = ahead(near, "ta", 1), ahead(far, "ta", 2)
    near_x, edge_x = ahead(near, "gx", 1), ahead(edge, "gx", 2)
    own2, near2, edge2 = call(
        lambda *refs: chain_kernel(n, *refs),
        [(12 * size, lanes), (10 * size, lanes), (10 * 2 * late, lanes)],
        [(18, 3 * n, lanes)],
        own,
        near_t,
        far_t,
    )
    near2_x, edge2_x = ahead(near2, "gx", 1), ahead(edge2, "gx", 2)
    transport = (RMAX * 18, block, lanes)
    spaces = lambda rows: [(12, rows + 2 * PAD, lanes), (12, rows + 2 * PAD, lanes), (12, rows, lanes)]
    early, packed = call(
        lambda *refs: early_kernel(n, *refs),
        [transport, (8, lanes)],
        [*spaces(block), (24, 8, lanes)],
        own,
        near_x,
        edge_x,
    )
    (packed,) = call(
        lambda *refs: late_kernel(n, *refs),
        [(16, lanes)],
        [*spaces(late * n), (RMAX * 18, (late + 1) * n, lanes)],
        own2,
        near2_x,
        edge2_x,
        early,
        packed,
    )
    count = lax.axis_size("gy")
    other = ahead(packed, "gy", 1) if count == 2 else lax.psum(packed, "gy") - packed
    scale = 1.0 / (3.0 * (lanes * count))
    (out,) = call(
        lambda *refs: last_kernel(n, scale, *refs),
        [(RMAX, n, n, TMAX)],
        [(RMAX, 4 * n, lanes)],
        packed,
        other,
    )
    return out.transpose(0, 3, 1, 2)


def shifted_2(block, axis, distance):
    devices = range(lax.axis_size(axis))
    route = [((i - distance) % len(devices), i) for i in devices]
    return lax.ppermute(block, axis, route)


def plain_times(left_mat, right_mat):
    real_rows = []
    imag_rows = []
    for i in range(3):
        real_cols = []
        imag_cols = []
        for k in range(3):
            real_sum = (
                left_mat[0, i, 0] * right_mat[0, 0, k] - left_mat[1, i, 0] * right_mat[1, 0, k]
            )
            imag_sum = (
                left_mat[0, i, 0] * right_mat[1, 0, k] + left_mat[1, i, 0] * right_mat[0, 0, k]
            )
            for j in range(1, 3):
                real_sum = (
                    real_sum
                    + left_mat[0, i, j] * right_mat[0, j, k]
                    - left_mat[1, i, j] * right_mat[1, j, k]
                )
                imag_sum = (
                    imag_sum
                    + left_mat[0, i, j] * right_mat[1, j, k]
                    + left_mat[1, i, j] * right_mat[0, j, k]
                )
            real_cols.append(real_sum)
            imag_cols.append(imag_sum)
        real_rows.append(jnp.stack(real_cols))
        imag_rows.append(jnp.stack(imag_cols))
    return jnp.stack([jnp.stack(real_rows), jnp.stack(imag_rows)])


def correlation(upper_half, lower_half):
    return jnp.sum(upper_half * lower_half, axis=(0, 1, 2, 5))


def next_x(field, along_dim):
    edge_cells = shifted_2(lax.slice_in_dim(field, 0, 1, axis=along_dim), "gx", -1)
    inner = lax.slice_in_dim(field, 1, field.shape[along_dim], axis=along_dim)
    return jnp.concatenate([inner, edge_cells], axis=along_dim)


def next_t(field):
    edge_cells = shifted_2(lax.slice_in_dim(field, 0, 1, axis=4), "ta", -1)
    inner = lax.slice_in_dim(field, 1, field.shape[4], axis=4)
    return jnp.concatenate([inner, edge_cells], axis=4)


def plain(link_x, link_t):
    all_rows = []
    temporal = [link_t]
    factor = link_t
    for _ in range(1, TMAX):
        factor = next_t(factor)
        temporal.append(plain_times(temporal[-1], factor))
    carried = jnp.stack(temporal)
    spatial = link_x
    factor_x = link_x
    for radius in range(RMAX):
        if radius > 0:
            factor_x = next_x(factor_x, 3)
            spatial = plain_times(spatial, factor_x)
        carried = next_x(carried, 4)
        shifted = spatial
        row_sums = []
        for extent in range(TMAX):
            shifted = next_t(shifted)
            upper_half = plain_times(spatial, carried[extent])
            lower_half = plain_times(temporal[extent], shifted)
            row_sums.append(correlation(upper_half, lower_half))
        all_rows.append(jnp.stack(row_sums))
    local_sums = jnp.stack(all_rows)
    totals = lax.psum(local_sums, "gy")
    return totals / (3.0 * (link_x.shape[5] * lax.axis_size("gy")))


def solution(mesh):
    return jax.shard_map(
        local,
        mesh=mesh,
        in_specs=(P(None, None, None, "gx", "ta", "gy"), P(None, None, None, "gx", "ta", "gy")),
        out_specs=P(None, None, "gx", "ta"),
        check_vma=False,
    )
```

```python
import jax
import jax.numpy as jnp
from jax import lax
from jax.experimental import pallas as pl
from jax.experimental.pallas import tpu as pltpu
from jax.sharding import PartitionSpec as P


RMAX = 6
TMAX = 6


def mul(a, b):
    return a[0] * b[0] - a[1] * b[1], a[0] * b[1] + a[1] * b[0]


def mul_conj(a, b):
    return a[0] * b[0] + a[1] * b[1], a[1] * b[0] - a[0] * b[1]


def add(a, b):
    return a[0] + b[0], a[1] + b[1]


def product(a, b):
    return [
        [add(add(mul(row[0], b[0][k]), mul(row[1], b[1][k])), mul(row[2], b[2][k])) for k in range(3)]
        for row in a
    ]


def product_dagger(a, b):
    return [
        [
            add(add(mul_conj(row[0], b[k][0]), mul_conj(row[1], b[k][1])), mul_conj(row[2], b[k][2]))
            for k in range(3)
        ]
        for row in a
    ]


def completed(a):
    last = []
    for k in range(3):
        i, j = (k + 1) % 3, (k + 2) % 3
        p, q = mul(a[0][i], a[1][j]), mul(a[0][j], a[1][i])
        last.append((p[0] - q[0], q[1] - p[1]))
    return [a[0], a[1], last]


def get(load, rows=2):
    return [[(load((3 * i + j) * 2), load((3 * i + j) * 2 + 1)) for j in range(3)] for i in range(rows)]


def put(store, a):
    for i, row in enumerate(a):
        for j in range(3):
            for k in range(2):
                store((3 * i + j) * 2 + k, row[j][k])


def where(mask, a, b):
    return [[tuple(jnp.where(mask, p, q) for p, q in zip(u, v)) for u, v in zip(r, s)] for r, s in zip(a, b)]


def unit(shape, rows=2):
    one, zero = jnp.ones(shape, jnp.float32), jnp.zeros(shape, jnp.float32)
    return [[(one if i == j else zero, zero) for j in range(3)] for i in range(rows)]


def pivots(y):
    sizes = [jnp.abs(v) for v in y]
    middle, end = jnp.maximum(sizes[1], sizes[2]), jnp.maximum(sizes[3], sizes[4])
    top = jnp.maximum(middle, end)
    other = jnp.logical_and(jnp.logical_and(top >= 0.35, top <= 1.5), sizes[0] <= 0.4)
    return jnp.logical_not(other), jnp.logical_and(other, end > middle)


def pick(mask, p, q):
    return tuple(jnp.where(mask, u, v) for u, v in zip(p, q))


VALUES = 8
TINY, FAR = 1e-30, 1e15


def projected(point):
    c, rest = point[0], point[1:]
    square = sum(v * v for v in rest)
    below = c < 0.0
    scale = jnp.where(below, 1.0 - c, 1.0) / jnp.where(below, jnp.maximum(square, TINY), 1.0 + c)
    y = [v * scale for v in rest]
    y[0] = jnp.where(jnp.logical_and(below, square < TINY), FAR, y[0])
    return y


def point_at(y):
    square = sum(v * v for v in y)
    inverse = 1.0 / (1.0 + square)
    v = [(1.0 - square) * inverse, *(v * (2.0 * inverse) for v in y)]
    return list(zip(v[0::2], v[1::2]))


def sent(m):
    y = projected([e for v in m[0] for e in v])
    b = m[1]
    first, last = pivots(y)
    w = [*pick(first, b[1], b[0]), *pick(last, b[1], b[2])]
    scale = lax.rsqrt(sum(v * v for v in w))
    return y + projected([v * scale for v in w])


def received(load):
    v = [load(k) for k in range(VALUES)]
    a = point_at(v[:5])
    e, f = point_at(v[5:])
    first, last = pivots(v[:5])
    p, q = pick(first, a[1], a[0]), pick(last, a[1], a[2])
    top = pick(first, a[0], pick(last, a[2], a[1]))
    scale = -1.0 / (top[0] * top[0] + top[1] * top[1])
    g = mul(add(mul_conj(e, p), mul_conj(f, q)), top)
    g = (g[0] * scale, g[1] * scale)
    norm = lax.rsqrt(1.0 + g[0] * g[0] + g[1] * g[1])
    e, f, g = [(u[0] * norm, u[1] * norm) for u in (e, f, g)]
    return [a, [pick(first, g, e), pick(first, e, pick(last, f, g)), pick(last, g, f)]]


def send(store, m):
    for k, e in enumerate(sent(m)):
        store(k, e)


def at_rows(ref, rows_of_value):
    def store(k, v):
        ref[rows_of_value(k)] = v

    return store


def flat_rows(ref, size, first, count, stride=None):
    rows = lambda k: pl.ds(k * size + first, count, stride=stride)
    return lambda k: ref[rows(k), :], at_rows(ref, rows)


def rows_of(ref, first, count, stride=None, offset=0):
    rows = pl.ds(first, count, stride=stride)
    return lambda k: ref[offset + k, rows, :], at_rows(ref, lambda k: (offset + k, rows))


def gauge_kernel(n, links_ref, own_ref, near_ref, far_ref, edge_ref, g_ref, u_ref):
    lanes = links_ref.shape[-1]
    block = n * n
    near, far, edge = block + 2 * n - 1, 2 * n + 1, 2 * n - 1

    def raw(field, t, rows):
        part = lambda p, i, j: links_ref[field, p * 9 + i * 3 + j, pl.ds(t, n, stride=n), :]
        return [[(part(0, i, j), part(1, i, j)) for j in range(3)] for i in range(rows)]

    g = unit((n, lanes))
    for t in range(n):
        put(rows_of(g_ref, t * n, n)[1], completed(g))
        full = raw(0, t, 3)
        put(rows_of(u_ref, t * n, n)[1], product(g, full) if t else full[:2])
        step = raw(1, t, 3)
        g = product(g, step) if t else step[:2]
    put(rows_of(own_ref, block + n, n)[1], g)
    send(flat_rows(near_ref, near, block, n)[1], g)
    g = get(rows_of(g_ref, 0, n, n)[0])
    put(rows_of(own_ref, block, n)[1], g)
    g = [[tuple(e[1:] for e in v) for v in row] for row in g]
    send(flat_rows(near_ref, near, block + n, n - 1)[1], g)
    last = lax.broadcasted_iota(jnp.int32, (8, lanes), 0) % n == n - 1
    for i in range(0, block, 8):
        after = where(last, unit((8, lanes), 3), get(rows_of(g_ref, i + 1, 8)[0], 3))
        w = product_dagger(get(rows_of(u_ref, i, 8)[0]), after)
        put(rows_of(own_ref, i, 8)[1], w)
        send(flat_rows(near_ref, near, i, 8)[1], w)
    for k in range(VALUES):
        far_ref[pl.ds(k * far, 2 * n), :] = near_ref[pl.ds(k * near, 2 * n), :]
        far_ref[pl.ds(k * far + 2 * n, 1), :] = near_ref[pl.ds(k * near + block + n, 1), :]
        edge_ref[pl.ds(k * edge, n), :] = near_ref[pl.ds(k * near, n, stride=n), :]
        edge_ref[pl.ds(k * edge + n, n - 1), :] = near_ref[pl.ds(k * near + block + n, n - 1), :]


def chain_kernel(n, own_ref, near_ref, far_ref, out_ref, late_ref, edge_ref, p_ref):
    lanes = own_ref.shape[-1]
    late, two, block = n + 2, 2 * n, n * n
    size = late * (n + 1)
    near, far = block + 2 * n - 1, 2 * n + 1

    def keep(first, count, m):
        put(flat_rows(out_ref, size, first, count)[1], m)
        send(flat_rows(late_ref, size, first, count)[1], m)

    def spread(p):
        p = completed(p)
        for k in range(3):
            put(rows_of(p_ref, k * n, n)[1], p)
        last = lax.broadcasted_iota(jnp.int32, (two, lanes), 0) % n == n - 1
        right = where(last, unit((two, lanes), 3), get(rows_of(p_ref, 1, two)[0], 3))
        return get(rows_of(p_ref, 0, two)[0]), right

    def first_of(p, count):
        return [[tuple(jnp.broadcast_to(e[0:1], (count, lanes)) for e in q) for q in row] for row in p]

    p = get(rows_of(own_ref, block + n, n)[0])
    p_next = received(flat_rows(near_ref, near, block, n)[0])
    pp = product(p, completed(p_next))
    left, right = spread(p)
    for i in range(0, block, 8):
        w = received(flat_rows(near_ref, near, i, 8)[0])
        keep(i, 8, product_dagger(product(left, completed(w)), right))
    keep(late * n, 1, first_of(p, 1))
    g = received(flat_rows(near_ref, near, block + n, n - 1)[0])
    keep(late * n + 1, n - 1, product(first_of(p, n - 1), completed(g)))
    left, right = spread(pp)
    w = received(flat_rows(far_ref, far, 0, two)[0])
    keep(block, two, product_dagger(product(left, completed(w)), right))
    keep(late * n + n, 1, first_of(pp, 1))
    g = received(flat_rows(far_ref, far, two, 1)[0])
    keep(late * n + n + 1, 1, product(first_of(pp, 1), completed(g)))
    for k in range(VALUES):
        edge_ref[pl.ds(k * 2 * late, late), :] = late_ref[pl.ds(k * size, late, stride=n), :]
        edge_ref[pl.ds(k * 2 * late + late, late), :] = late_ref[pl.ds(k * size + late * n, late), :]


PAD = 8


def transports(n, times, a_ref, b_ref, c_ref, closing, store):
    lanes = a_ref.shape[-1]
    for ref, g in zip((a_ref, b_ref), closing):
        load, keep = rows_of(ref, PAD + n - 1, times, n)
        put(keep, product_dagger(get(load), completed(g)))
    x_of = lax.broadcasted_iota(jnp.int32, (8, lanes), 0) % n

    def window(k, i):
        own = lambda shift: get(rows_of(a_ref, PAD + i + shift, 8)[0])
        after = lambda shift: get(rows_of(b_ref, PAD + i + shift, 8)[0])
        if k == 0:
            return own(0)
        if k < n:
            return where(x_of < n - k, own(k), after(k - n))
        if k == n:
            return after(0)
        return where(x_of < n - 1, after(1), get(rows_of(c_ref, i, 8)[0]))

    for i in range(0, times * n, 8):
        s = window(0, i)
        for r in range(RMAX):
            if r:
                s = product(s, completed(window(r, i)))
            put(lambda c, v: store(r * 18 + c, i, v), completed(s))


def paired(pairs, at):
    sums = [None] * len(pairs)
    for c in range(18):
        for k, (p, q) in enumerate(pairs):
            e = at(c, p) * at(c, q)
            sums[k] = e if c == 0 else sums[k] + e
    return [jnp.sum(v, axis=1, keepdims=True) for v in sums]


def early_kernel(n, own_ref, near_ref, far_ref, s_ref, out_ref, a_ref, b_ref, c_ref, g_ref):
    lanes = own_ref.shape[-1]
    block = n * n
    near, edge = block + 2 * n - 1, 2 * n - 1
    for i in range(0, block, 8):
        put(rows_of(a_ref, PAD + i, 8)[1], get(rows_of(own_ref, i, 8)[0]))
        put(rows_of(b_ref, PAD + i, 8)[1], received(flat_rows(near_ref, near, i, 8)[0]))
    put(rows_of(c_ref, n - 1, n, n)[1], received(flat_rows(far_ref, edge, 0, n)[0]))
    closing = []
    for k, load in enumerate((flat_rows(near_ref, near, block + n, n - 1), flat_rows(far_ref, edge, n, n - 1))):
        put(rows_of(g_ref, 0, 1, offset=12 * k)[1], unit((1, lanes)))
        put(rows_of(g_ref, 1, n - 1, offset=12 * k)[1], received(load[0]))
        closing.append(get(rows_of(g_ref, 0, n, offset=12 * k)[0]))

    def store(c, i, v):
        s_ref[c, pl.ds(i, 8), :] = v

    transports(n, n, a_ref, b_ref, c_ref, closing, store)
    lane = lax.broadcasted_iota(jnp.int32, (8, lanes), 1)
    packed = jnp.zeros((8, lanes), jnp.float32)
    for r in range(RMAX):
        at = lambda c, t: s_ref[r * 18 + c, pl.ds(t * n, 8), :]
        for u, total in enumerate(paired([(0, 1), (0, 2)], at)):
            packed = jnp.where(lane == r * TMAX + u, total, packed)
    out_ref[...] = packed


def late_kernel(n, own_ref, near_ref, far_ref, early_ref, packed_ref, out_ref, a_ref, b_ref, c_ref, s_ref):
    lanes = own_ref.shape[-1]
    late = n + 2
    size = late * (n + 1)
    for i in range(0, late * n, 8):
        put(rows_of(a_ref, PAD + i, 8)[1], get(flat_rows(own_ref, size, i, 8)[0]))
        put(rows_of(b_ref, PAD + i, 8)[1], received(flat_rows(near_ref, size, i, 8)[0]))
    put(rows_of(c_ref, n - 1, late, n)[1], received(flat_rows(far_ref, 2 * late, 0, late)[0]))
    closing = [
        received(flat_rows(near_ref, size, late * n, late)[0]),
        received(flat_rows(far_ref, 2 * late, late, late)[0]),
    ]

    def store(c, i, v):
        s_ref[c, pl.ds(n + i, 8), :] = v

    transports(n, late, a_ref, b_ref, c_ref, closing, store)
    for c in range(RMAX * 18):
        s_ref[c, pl.ds(0, n), :] = early_ref[c, pl.ds(n * n - n, n), :]
    lane = lax.broadcasted_iota(jnp.int32, (8, lanes), 1)
    packed = [packed_ref[...], jnp.zeros((8, lanes), jnp.float32)]
    places = [(h, u) for u in range(1, TMAX + 1) for h in range(2) if (h, u) not in ((0, 1), (0, 2))]
    for r in range(RMAX):

        def at(c, t):
            if t < n - 1:
                return early_ref[r * 18 + c, pl.ds(t * n, 8), :]
            return s_ref[r * 18 + c, pl.ds((t - n + 1) * n, 8), :]

        for (h, u), total in zip(places, paired([(2 * h, 2 * h + u) for h, u in places], at)):
            packed[h] = jnp.where(lane == r * TMAX + u - 1, total, packed[h])
    for h in range(2):
        out_ref[pl.ds(8 * h, 8), :] = packed[h]


def last_kernel(n, scale, own_ref, other_ref, out_ref, v_ref):
    lanes = own_ref.shape[-1]
    total = (own_ref[...] + other_ref[...]) * scale
    for r in range(RMAX):
        v_ref[r] = pltpu.roll(total, lanes - r * TMAX, 1) if r else total
        for x in range(n):
            out_ref[r, x] = v_ref[r, pl.ds(x, n, stride=n), :][:, :TMAX]


def call(kernel, outs, scratch, *args, space=pltpu.VMEM):
    return pl.pallas_call(
        kernel,
        out_shape=[jax.ShapeDtypeStruct(s, jnp.float32) for s in outs],
        in_specs=[pl.BlockSpec(memory_space=space)] * len(args),
        out_specs=[pl.BlockSpec(memory_space=pltpu.VMEM)] * len(outs),
        scratch_shapes=[pltpu.VMEM(s, jnp.float32) if isinstance(s, tuple) else s for s in scratch],
        compiler_params=pltpu.CompilerParams(vmem_limit_bytes=8 * 2**20),
    )(*args)


def ahead(block, axis, distance):
    count = lax.axis_size(axis)
    return lax.ppermute(block, axis, [((i + distance) % count, i) for i in range(count)])


def local(link_x, link_t):
    n, lanes = link_x.shape[3], link_x.shape[5]
    if (n, link_x.shape[4], lanes) != (4, 4, 128):
        return plain(link_x, link_t)
    late, block = n + 2, n * n
    size, two = late * (n + 1), 2 * n
    flat = (18, block, lanes)
    own, near, far, edge = call(
        lambda *refs: gauge_kernel(n, *refs),
        [(12, block + two, lanes)] + [(VALUES * rows, lanes) for rows in (block + two - 1, two + 1, two - 1)],
        [(18, block + 8, lanes), (12, block, lanes)],
        jnp.stack([link_x.reshape(flat), link_t.reshape(flat)]),
    )
    near_t, far_t = ahead(near, "ta", 1), ahead(far, "ta", 2)
    near_x, edge_x = ahead(near, "gx", 1), ahead(edge, "gx", 2)
    own2, near2, edge2 = call(
        lambda *refs: chain_kernel(n, *refs),
        [(12 * size, lanes), (VALUES * size, lanes), (VALUES * 2 * late, lanes)],
        [(18, 3 * n, lanes)],
        own,
        near_t,
        far_t,
    )
    near2_x, edge2_x = ahead(near2, "gx", 1), ahead(edge2, "gx", 2)
    transport = (RMAX * 18, block, lanes)
    spaces = lambda rows: [(12, rows + 2 * PAD, lanes), (12, rows + 2 * PAD, lanes), (12, rows, lanes)]
    early, packed = call(
        lambda *refs: early_kernel(n, *refs),
        [transport, (8, lanes)],
        [*spaces(block), (24, 8, lanes)],
        own,
        near_x,
        edge_x,
    )
    (packed,) = call(
        lambda *refs: late_kernel(n, *refs),
        [(16, lanes)],
        [*spaces(late * n), (RMAX * 18, (late + 1) * n, lanes)],
        own2,
        near2_x,
        edge2_x,
        early,
        packed,
    )
    count = lax.axis_size("gy")
    other = ahead(packed, "gy", 1) if count == 2 else lax.psum(packed, "gy") - packed
    scale = 1.0 / (3.0 * (lanes * count))
    (out,) = call(
        lambda *refs: last_kernel(n, scale, *refs),
        [(RMAX, n, n, TMAX)],
        [(RMAX, 4 * n, lanes)],
        packed,
        other,
    )
    return out.transpose(0, 3, 1, 2)


def shifted_2(block, axis, distance):
    devices = range(lax.axis_size(axis))
    route = [((i - distance) % len(devices), i) for i in devices]
    return lax.ppermute(block, axis, route)


def plain_times(left_mat, right_mat):
    real_rows = []
    imag_rows = []
    for i in range(3):
        real_cols = []
        imag_cols = []
        for k in range(3):
            real_sum = (
                left_mat[0, i, 0] * right_mat[0, 0, k] - left_mat[1, i, 0] * right_mat[1, 0, k]
            )
            imag_sum = (
                left_mat[0, i, 0] * right_mat[1, 0, k] + left_mat[1, i, 0] * right_mat[0, 0, k]
            )
            for j in range(1, 3):
                real_sum = (
                    real_sum
                    + left_mat[0, i, j] * right_mat[0, j, k]
                    - left_mat[1, i, j] * right_mat[1, j, k]
                )
                imag_sum = (
                    imag_sum
                    + left_mat[0, i, j] * right_mat[1, j, k]
                    + left_mat[1, i, j] * right_mat[0, j, k]
                )
            real_cols.append(real_sum)
            imag_cols.append(imag_sum)
        real_rows.append(jnp.stack(real_cols))
        imag_rows.append(jnp.stack(imag_cols))
    return jnp.stack([jnp.stack(real_rows), jnp.stack(imag_rows)])


def correlation(upper_half, lower_half):
    return jnp.sum(upper_half * lower_half, axis=(0, 1, 2, 5))


def next_x(field, along_dim):
    edge_cells = shifted_2(lax.slice_in_dim(field, 0, 1, axis=along_dim), "gx", -1)
    inner = lax.slice_in_dim(field, 1, field.shape[along_dim], axis=along_dim)
    return jnp.concatenate([inner, edge_cells], axis=along_dim)


def next_t(field):
    edge_cells = shifted_2(lax.slice_in_dim(field, 0, 1, axis=4), "ta", -1)
    inner = lax.slice_in_dim(field, 1, field.shape[4], axis=4)
    return jnp.concatenate([inner, edge_cells], axis=4)


def plain(link_x, link_t):
    all_rows = []
    temporal = [link_t]
    factor = link_t
    for _ in range(1, TMAX):
        factor = next_t(factor)
        temporal.append(plain_times(temporal[-1], factor))
    carried = jnp.stack(temporal)
    spatial = link_x
    factor_x = link_x
    for radius in range(RMAX):
        if radius > 0:
            factor_x = next_x(factor_x, 3)
            spatial = plain_times(spatial, factor_x)
        carried = next_x(carried, 4)
        shifted = spatial
        row_sums = []
        for extent in range(TMAX):
            shifted = next_t(shifted)
            upper_half = plain_times(spatial, carried[extent])
            lower_half = plain_times(temporal[extent], shifted)
            row_sums.append(correlation(upper_half, lower_half))
        all_rows.append(jnp.stack(row_sums))
    local_sums = jnp.stack(all_rows)
    totals = lax.psum(local_sums, "gy")
    return totals / (3.0 * (link_x.shape[5] * lax.axis_size("gy")))


def solution(mesh):
    return jax.shard_map(
        local,
        mesh=mesh,
        in_specs=(P(None, None, None, "gx", "ta", "gy"), P(None, None, None, "gx", "ta", "gy")),
        out_specs=P(None, None, "gx", "ta"),
        check_vma=False,
    )
```

```python
import jax
import jax.numpy as jnp
from jax import lax
from jax.experimental import pallas as pl
from jax.experimental.pallas import tpu as pltpu
from jax.sharding import PartitionSpec as P


RMAX = 6
TMAX = 6


def mul(a, b):
    return a[0] * b[0] - a[1] * b[1], a[0] * b[1] + a[1] * b[0]


def mul_conj(a, b):
    return a[0] * b[0] + a[1] * b[1], a[1] * b[0] - a[0] * b[1]


def add(a, b):
    return a[0] + b[0], a[1] + b[1]


def product(a, b):
    return [
        [add(add(mul(row[0], b[0][k]), mul(row[1], b[1][k])), mul(row[2], b[2][k])) for k in range(3)]
        for row in a
    ]


def product_dagger(a, b):
    return [
        [
            add(add(mul_conj(row[0], b[k][0]), mul_conj(row[1], b[k][1])), mul_conj(row[2], b[k][2]))
            for k in range(3)
        ]
        for row in a
    ]


def completed(a):
    last = []
    for k in range(3):
        i, j = (k + 1) % 3, (k + 2) % 3
        p, q = mul(a[0][i], a[1][j]), mul(a[0][j], a[1][i])
        last.append((p[0] - q[0], q[1] - p[1]))
    return [a[0], a[1], last]


def get(load, rows=2):
    return [[(load((3 * i + j) * 2), load((3 * i + j) * 2 + 1)) for j in range(3)] for i in range(rows)]


def put(store, a):
    for i, row in enumerate(a):
        for j in range(3):
            for k in range(2):
                store((3 * i + j) * 2 + k, row[j][k])


def where(mask, a, b):
    return [[tuple(jnp.where(mask, p, q) for p, q in zip(u, v)) for u, v in zip(r, s)] for r, s in zip(a, b)]


def unit(shape, rows=2):
    one, zero = jnp.ones(shape, jnp.float32), jnp.zeros(shape, jnp.float32)
    return [[(one if i == j else zero, zero) for j in range(3)] for i in range(rows)]


def pivots(y):
    sizes = [jnp.abs(v) for v in y]
    middle, end = jnp.maximum(sizes[1], sizes[2]), jnp.maximum(sizes[3], sizes[4])
    top = jnp.maximum(middle, end)
    other = jnp.logical_and(jnp.logical_and(top >= 0.35, top <= 1.5), sizes[0] <= 0.4)
    return jnp.logical_not(other), jnp.logical_and(other, end > middle)


def pick(mask, p, q):
    return tuple(jnp.where(mask, u, v) for u, v in zip(p, q))


VALUES = 8
TINY, FAR = 1e-30, 1e15


def projected(point):
    c, rest = point[0], point[1:]
    square = sum(v * v for v in rest)
    below = c < 0.0
    scale = jnp.where(below, 1.0 - c, 1.0) / jnp.where(below, jnp.maximum(square, TINY), 1.0 + c)
    y = [v * scale for v in rest]
    y[0] = jnp.where(jnp.logical_and(below, square < TINY), FAR, y[0])
    return y


def point_at(y):
    square = sum(v * v for v in y)
    inverse = 1.0 / (1.0 + square)
    v = [(1.0 - square) * inverse, *(v * (2.0 * inverse) for v in y)]
    return list(zip(v[0::2], v[1::2]))


def sent(m):
    y = projected([e for v in m[0] for e in v])
    b = m[1]
    first, last = pivots(y)
    w = [*pick(first, b[1], b[0]), *pick(last, b[1], b[2])]
    scale = lax.rsqrt(sum(v * v for v in w))
    return y + projected([v * scale for v in w])


def received(load):
    v = [load(k) for k in range(VALUES)]
    a = point_at(v[:5])
    e, f = point_at(v[5:])
    first, last = pivots(v[:5])
    p, q = pick(first, a[1], a[0]), pick(last, a[1], a[2])
    top = pick(first, a[0], pick(last, a[2], a[1]))
    scale = -1.0 / (top[0] * top[0] + top[1] * top[1])
    g = mul(add(mul_conj(e, p), mul_conj(f, q)), top)
    g = (g[0] * scale, g[1] * scale)
    norm = lax.rsqrt(1.0 + g[0] * g[0] + g[1] * g[1])
    e, f, g = [(u[0] * norm, u[1] * norm) for u in (e, f, g)]
    return [a, [pick(first, g, e), pick(first, e, pick(last, f, g)), pick(last, g, f)]]


def send(store, m):
    for k, e in enumerate(sent(m)):
        store(k, e)


def at_rows(ref, rows_of_value):
    def store(k, v):
        ref[rows_of_value(k)] = v

    return store


def flat_rows(ref, size, first, count, stride=None):
    rows = lambda k: pl.ds(k * size + first, count, stride=stride)
    return lambda k: ref[rows(k), :], at_rows(ref, rows)


def rows_of(ref, first, count, stride=None, offset=0):
    rows = pl.ds(first, count, stride=stride)
    return lambda k: ref[offset + k, rows, :], at_rows(ref, lambda k: (offset + k, rows))


def gauge_kernel(n, links_ref, own_ref, near_ref, far_ref, edge_ref, g_ref, u_ref):
    lanes = links_ref.shape[-1]
    block = n * n
    near, far, edge = block + 2 * n - 1, 2 * n + 1, 2 * n - 1

    def raw(field, t, rows):
        part = lambda p, i, j: links_ref[field, p * 9 + i * 3 + j, pl.ds(t, n, stride=n), :]
        return [[(part(0, i, j), part(1, i, j)) for j in range(3)] for i in range(rows)]

    g = unit((n, lanes))
    for t in range(n):
        put(rows_of(g_ref, t * n, n)[1], completed(g))
        full = raw(0, t, 3)
        put(rows_of(u_ref, t * n, n)[1], product(g, full) if t else full[:2])
        step = raw(1, t, 3)
        g = product(g, step) if t else step[:2]
    put(rows_of(own_ref, block, n)[1], g)
    put(rows_of(own_ref, block + n, n - 1)[1], get(rows_of(g_ref, n, n - 1, n)[0]))
    send(flat_rows(near_ref, near, block, 2 * n - 1)[1], get(rows_of(own_ref, block, 2 * n - 1)[0]))
    last = lax.broadcasted_iota(jnp.int32, (8, lanes), 0) % n == n - 1
    for i in range(0, block, 8):
        after = where(last, unit((8, lanes), 3), get(rows_of(g_ref, i + 1, 8)[0], 3))
        w = product_dagger(get(rows_of(u_ref, i, 8)[0]), after)
        put(rows_of(own_ref, i, 8)[1], w)
        send(flat_rows(near_ref, near, i, 8)[1], w)
    for k in range(VALUES):
        far_ref[pl.ds(k * far, 2 * n), :] = near_ref[pl.ds(k * near, 2 * n), :]
        far_ref[pl.ds(k * far + 2 * n, 1), :] = near_ref[pl.ds(k * near + block + n, 1), :]
        edge_ref[pl.ds(k * edge, n), :] = near_ref[pl.ds(k * near, n, stride=n), :]
        edge_ref[pl.ds(k * edge + n, n - 1), :] = near_ref[pl.ds(k * near + block + n, n - 1), :]


def chain_kernel(n, own_ref, near_ref, far_ref, out_ref, late_ref, edge_ref, p_ref):
    lanes = own_ref.shape[-1]
    late, two, block = n + 2, 2 * n, n * n
    size = late * (n + 1)
    near, far = block + 2 * n - 1, 2 * n + 1

    def keep(first, count, m):
        put(flat_rows(out_ref, size, first, count)[1], m)
        send(flat_rows(late_ref, size, first, count)[1], m)

    def spread(p):
        p = completed(p)
        for k in range(3):
            put(rows_of(p_ref, k * n, n)[1], p)
        last = lax.broadcasted_iota(jnp.int32, (two, lanes), 0) % n == n - 1
        right = where(last, unit((two, lanes), 3), get(rows_of(p_ref, 1, two)[0], 3))
        return get(rows_of(p_ref, 0, two)[0]), right

    def first_of(p, count):
        return [[tuple(jnp.broadcast_to(e[0:1], (count, lanes)) for e in q) for q in row] for row in p]

    p = get(rows_of(own_ref, block, n)[0])
    p_next = received(flat_rows(near_ref, near, block, n)[0])
    pp = product(p, completed(p_next))
    hold = lambda first, count, m: put(flat_rows(out_ref, size, first, count)[1], m)
    hold(late * n, 1, first_of(p, 1))
    g = received(flat_rows(near_ref, near, block + n, n - 1)[0])
    hold(late * n + 1, n - 1, product(first_of(p, n - 1), completed(g)))
    hold(late * n + n, 1, first_of(pp, 1))
    g = received(flat_rows(far_ref, far, two, 1)[0])
    hold(late * n + n + 1, 1, product(first_of(pp, 1), completed(g)))
    left, right = spread(p)
    for i in range(0, block, 8):
        w = received(flat_rows(near_ref, near, i, 8)[0])
        keep(i, 8, product_dagger(product(left, completed(w)), right))
    left, right = spread(pp)
    w = received(flat_rows(far_ref, far, 0, two)[0])
    keep(block, two, product_dagger(product(left, completed(w)), right))
    send(flat_rows(late_ref, size, late * n, late)[1], get(flat_rows(out_ref, size, late * n, late)[0]))
    for k in range(VALUES):
        edge_ref[pl.ds(k * 2 * late, late), :] = late_ref[pl.ds(k * size, late, stride=n), :]
        edge_ref[pl.ds(k * 2 * late + late, late), :] = late_ref[pl.ds(k * size + late * n, late), :]


PAD = 8


def transports(n, times, a_ref, b_ref, c_ref, closing, store):
    lanes = a_ref.shape[-1]
    for ref, g in zip((a_ref, b_ref), closing):
        load, keep = rows_of(ref, PAD + n - 1, times, n)
        put(keep, completed(product_dagger(get(load), completed(g))))
    x_of = lax.broadcasted_iota(jnp.int32, (8, lanes), 0) % n

    def window(k, i):
        own = lambda shift: get(rows_of(a_ref, PAD + i + shift, 8)[0], 3)
        after = lambda shift: get(rows_of(b_ref, PAD + i + shift, 8)[0], 3)
        if k == 0:
            return own(0)
        if k < n:
            return where(x_of < n - k, own(k), after(k - n))
        if k == n:
            return after(0)
        return where(x_of < n - 1, after(1), get(rows_of(c_ref, i, 8)[0], 3))

    for i in range(0, times * n, 8):
        s = window(0, i)[:2]
        for r in range(RMAX):
            if r:
                s = product(s, window(r, i))
            put(lambda c, v: store(r * 18 + c, i, v), completed(s))


def paired(pairs, at):
    sums = [None] * len(pairs)
    for c in range(18):
        for k, (p, q) in enumerate(pairs):
            e = at(c, p) * at(c, q)
            sums[k] = e if c == 0 else sums[k] + e
    return [jnp.sum(v, axis=1, keepdims=True) for v in sums]


def early_kernel(n, own_ref, near_ref, far_ref, s_ref, out_ref, a_ref, b_ref, c_ref, g_ref):
    lanes = own_ref.shape[-1]
    block = n * n
    near, edge = block + 2 * n - 1, 2 * n - 1
    for i in range(0, block, 8):
        put(rows_of(a_ref, PAD + i, 8)[1], completed(get(rows_of(own_ref, i, 8)[0])))
        put(rows_of(b_ref, PAD + i, 8)[1], completed(received(flat_rows(near_ref, near, i, 8)[0])))
    put(rows_of(c_ref, n - 1, n, n)[1], completed(received(flat_rows(far_ref, edge, 0, n)[0])))
    closing = []
    for k, load in enumerate((flat_rows(near_ref, near, block + n, n - 1), flat_rows(far_ref, edge, n, n - 1))):
        put(rows_of(g_ref, 0, 1, offset=12 * k)[1], unit((1, lanes)))
        put(rows_of(g_ref, 1, n - 1, offset=12 * k)[1], received(load[0]))
        closing.append(get(rows_of(g_ref, 0, n, offset=12 * k)[0]))

    def store(c, i, v):
        s_ref[c, pl.ds(i, 8), :] = v

    transports(n, n, a_ref, b_ref, c_ref, closing, store)
    lane = lax.broadcasted_iota(jnp.int32, (8, lanes), 1)
    packed = jnp.zeros((8, lanes), jnp.float32)
    for r in range(RMAX):
        at = lambda c, t: s_ref[r * 18 + c, pl.ds(t * n, 8), :]
        for u, total in enumerate(paired([(0, 1), (0, 2)], at)):
            packed = jnp.where(lane == r * TMAX + u, total, packed)
    out_ref[...] = packed


def late_kernel(n, own_ref, near_ref, far_ref, early_ref, packed_ref, out_ref, a_ref, b_ref, c_ref, s_ref):
    lanes = own_ref.shape[-1]
    late = n + 2
    size = late * (n + 1)
    for i in range(0, late * n, 8):
        put(rows_of(a_ref, PAD + i, 8)[1], completed(get(flat_rows(own_ref, size, i, 8)[0])))
        put(rows_of(b_ref, PAD + i, 8)[1], completed(received(flat_rows(near_ref, size, i, 8)[0])))
    put(rows_of(c_ref, n - 1, late, n)[1], completed(received(flat_rows(far_ref, 2 * late, 0, late)[0])))
    closing = [
        received(flat_rows(near_ref, size, late * n, late)[0]),
        received(flat_rows(far_ref, 2 * late, late, late)[0]),
    ]

    def store(c, i, v):
        s_ref[c, pl.ds(n + i, 8), :] = v

    transports(n, late, a_ref, b_ref, c_ref, closing, store)
    for c in range(RMAX * 18):
        s_ref[c, pl.ds(0, n), :] = early_ref[c, pl.ds(n * n - n, n), :]
    lane = lax.broadcasted_iota(jnp.int32, (8, lanes), 1)
    packed = [packed_ref[...], jnp.zeros((8, lanes), jnp.float32)]
    places = [(h, u) for u in range(1, TMAX + 1) for h in range(2) if (h, u) not in ((0, 1), (0, 2))]
    for r in range(RMAX):

        def at(c, t):
            if t < n - 1:
                return early_ref[r * 18 + c, pl.ds(t * n, 8), :]
            return s_ref[r * 18 + c, pl.ds((t - n + 1) * n, 8), :]

        for (h, u), total in zip(places, paired([(2 * h, 2 * h + u) for h, u in places], at)):
            packed[h] = jnp.where(lane == r * TMAX + u - 1, total, packed[h])
    for h in range(2):
        out_ref[pl.ds(8 * h, 8), :] = packed[h]


def last_kernel(n, scale, own_ref, other_ref, out_ref, v_ref):
    lanes = own_ref.shape[-1]
    total = (own_ref[...] + other_ref[...]) * scale
    for r in range(RMAX):
        v_ref[r] = pltpu.roll(total, lanes - r * TMAX, 1) if r else total
        for x in range(n):
            out_ref[r, x] = v_ref[r, pl.ds(x, n, stride=n), :][:, :TMAX]


def call(kernel, outs, scratch, *args, space=pltpu.VMEM):
    return pl.pallas_call(
        kernel,
        out_shape=[jax.ShapeDtypeStruct(s, jnp.float32) for s in outs],
        in_specs=[pl.BlockSpec(memory_space=space)] * len(args),
        out_specs=[pl.BlockSpec(memory_space=pltpu.VMEM)] * len(outs),
        scratch_shapes=[pltpu.VMEM(s, jnp.float32) if isinstance(s, tuple) else s for s in scratch],
        compiler_params=pltpu.CompilerParams(vmem_limit_bytes=8 * 2**20),
    )(*args)


def ahead(block, axis, distance):
    count = lax.axis_size(axis)
    return lax.ppermute(block, axis, [((i + distance) % count, i) for i in range(count)])


def local(link_x, link_t):
    n, lanes = link_x.shape[3], link_x.shape[5]
    if (n, link_x.shape[4], lanes) != (4, 4, 128):
        return plain(link_x, link_t)
    late, block = n + 2, n * n
    size, two = late * (n + 1), 2 * n
    flat = (18, block, lanes)
    own, near, far, edge = call(
        lambda *refs: gauge_kernel(n, *refs),
        [(12, block + two, lanes)] + [(VALUES * rows, lanes) for rows in (block + two - 1, two + 1, two - 1)],
        [(18, block + 8, lanes), (12, block, lanes)],
        jnp.stack([link_x.reshape(flat), link_t.reshape(flat)]),
    )
    near_t, far_t = ahead(near, "ta", 1), ahead(far, "ta", 2)
    near_x, edge_x = ahead(near, "gx", 1), ahead(edge, "gx", 2)
    own2, near2, edge2 = call(
        lambda *refs: chain_kernel(n, *refs),
        [(12 * size, lanes), (VALUES * size, lanes), (VALUES * 2 * late, lanes)],
        [(18, 3 * n, lanes)],
        own,
        near_t,
        far_t,
    )
    near2_x, edge2_x = ahead(near2, "gx", 1), ahead(edge2, "gx", 2)
    transport = (RMAX * 18, block, lanes)
    spaces = lambda rows: [(18, rows + 2 * PAD, lanes), (18, rows + 2 * PAD, lanes), (18, rows, lanes)]
    early, packed = call(
        lambda *refs: early_kernel(n, *refs),
        [transport, (8, lanes)],
        [*spaces(block), (24, 8, lanes)],
        own,
        near_x,
        edge_x,
    )
    (packed,) = call(
        lambda *refs: late_kernel(n, *refs),
        [(16, lanes)],
        [*spaces(late * n), (RMAX * 18, (late + 1) * n, lanes)],
        own2,
        near2_x,
        edge2_x,
        early,
        packed,
    )
    count = lax.axis_size("gy")
    other = ahead(packed, "gy", 1) if count == 2 else lax.psum(packed, "gy") - packed
    scale = 1.0 / (3.0 * (lanes * count))
    (out,) = call(
        lambda *refs: last_kernel(n, scale, *refs),
        [(RMAX, n, n, TMAX)],
        [(RMAX, 4 * n, lanes)],
        packed,
        other,
    )
    return out.transpose(0, 3, 1, 2)


def shifted_2(block, axis, distance):
    devices = range(lax.axis_size(axis))
    route = [((i - distance) % len(devices), i) for i in devices]
    return lax.ppermute(block, axis, route)


def plain_times(left_mat, right_mat):
    real_rows = []
    imag_rows = []
    for i in range(3):
        real_cols = []
        imag_cols = []
        for k in range(3):
            real_sum = (
                left_mat[0, i, 0] * right_mat[0, 0, k] - left_mat[1, i, 0] * right_mat[1, 0, k]
            )
            imag_sum = (
                left_mat[0, i, 0] * right_mat[1, 0, k] + left_mat[1, i, 0] * right_mat[0, 0, k]
            )
            for j in range(1, 3):
                real_sum = (
                    real_sum
                    + left_mat[0, i, j] * right_mat[0, j, k]
                    - left_mat[1, i, j] * right_mat[1, j, k]
                )
                imag_sum = (
                    imag_sum
                    + left_mat[0, i, j] * right_mat[1, j, k]
                    + left_mat[1, i, j] * right_mat[0, j, k]
                )
            real_cols.append(real_sum)
            imag_cols.append(imag_sum)
        real_rows.append(jnp.stack(real_cols))
        imag_rows.append(jnp.stack(imag_cols))
    return jnp.stack([jnp.stack(real_rows), jnp.stack(imag_rows)])


def correlation(upper_half, lower_half):
    return jnp.sum(upper_half * lower_half, axis=(0, 1, 2, 5))


def next_x(field, along_dim):
    edge_cells = shifted_2(lax.slice_in_dim(field, 0, 1, axis=along_dim), "gx", -1)
    inner = lax.slice_in_dim(field, 1, field.shape[along_dim], axis=along_dim)
    return jnp.concatenate([inner, edge_cells], axis=along_dim)


def next_t(field):
    edge_cells = shifted_2(lax.slice_in_dim(field, 0, 1, axis=4), "ta", -1)
    inner = lax.slice_in_dim(field, 1, field.shape[4], axis=4)
    return jnp.concatenate([inner, edge_cells], axis=4)


def plain(link_x, link_t):
    all_rows = []
    temporal = [link_t]
    factor = link_t
    for _ in range(1, TMAX):
        factor = next_t(factor)
        temporal.append(plain_times(temporal[-1], factor))
    carried = jnp.stack(temporal)
    spatial = link_x
    factor_x = link_x
    for radius in range(RMAX):
        if radius > 0:
            factor_x = next_x(factor_x, 3)
            spatial = plain_times(spatial, factor_x)
        carried = next_x(carried, 4)
        shifted = spatial
        row_sums = []
        for extent in range(TMAX):
            shifted = next_t(shifted)
            upper_half = plain_times(spatial, carried[extent])
            lower_half = plain_times(temporal[extent], shifted)
            row_sums.append(correlation(upper_half, lower_half))
        all_rows.append(jnp.stack(row_sums))
    local_sums = jnp.stack(all_rows)
    totals = lax.psum(local_sums, "gy")
    return totals / (3.0 * (link_x.shape[5] * lax.axis_size("gy")))


def solution(mesh):
    return jax.shard_map(
        local,
        mesh=mesh,
        in_specs=(P(None, None, None, "gx", "ta", "gy"), P(None, None, None, "gx", "ta", "gy")),
        out_specs=P(None, None, "gx", "ta"),
        check_vma=False,
    )
```

```python
import jax
import jax.numpy as jnp
from jax import lax
from jax.experimental import pallas as pl
from jax.experimental.pallas import tpu as pltpu
from jax.sharding import PartitionSpec as P


RMAX = 6
TMAX = 6


def mul(a, b):
    return a[0] * b[0] - a[1] * b[1], a[0] * b[1] + a[1] * b[0]


def mul_conj(a, b):
    return a[0] * b[0] + a[1] * b[1], a[1] * b[0] - a[0] * b[1]


def add(a, b):
    return a[0] + b[0], a[1] + b[1]


def product(a, b):
    return [
        [add(add(mul(row[0], b[0][k]), mul(row[1], b[1][k])), mul(row[2], b[2][k])) for k in range(3)]
        for row in a
    ]


def product_dagger(a, b):
    return [
        [
            add(add(mul_conj(row[0], b[k][0]), mul_conj(row[1], b[k][1])), mul_conj(row[2], b[k][2]))
            for k in range(3)
        ]
        for row in a
    ]


def completed(a):
    last = []
    for k in range(3):
        i, j = (k + 1) % 3, (k + 2) % 3
        p, q = mul(a[0][i], a[1][j]), mul(a[0][j], a[1][i])
        last.append((p[0] - q[0], q[1] - p[1]))
    return [a[0], a[1], last]


def get(load, rows=2):
    return [[(load((3 * i + j) * 2), load((3 * i + j) * 2 + 1)) for j in range(3)] for i in range(rows)]


def put(store, a):
    for i, row in enumerate(a):
        for j in range(3):
            for k in range(2):
                store((3 * i + j) * 2 + k, row[j][k])


def where(mask, a, b):
    return [[tuple(jnp.where(mask, p, q) for p, q in zip(u, v)) for u, v in zip(r, s)] for r, s in zip(a, b)]


def unit(shape, rows=2):
    one, zero = jnp.ones(shape, jnp.float32), jnp.zeros(shape, jnp.float32)
    return [[(one if i == j else zero, zero) for j in range(3)] for i in range(rows)]


def pivots(y):
    sizes = [jnp.abs(v) for v in y]
    middle, end = jnp.maximum(sizes[1], sizes[2]), jnp.maximum(sizes[3], sizes[4])
    top = jnp.maximum(middle, end)
    other = jnp.logical_and(jnp.logical_and(top >= 0.35, top <= 1.5), sizes[0] <= 0.4)
    return jnp.logical_not(other), jnp.logical_and(other, end > middle)


def pick(mask, p, q):
    return tuple(jnp.where(mask, u, v) for u, v in zip(p, q))


VALUES = 8
TINY, FAR = 1e-30, 1e15


def projected(point):
    c, rest = point[0], point[1:]
    square = sum(v * v for v in rest)
    below = c < 0.0
    scale = jnp.where(below, 1.0 - c, 1.0) / jnp.where(below, jnp.maximum(square, TINY), 1.0 + c)
    y = [v * scale for v in rest]
    y[0] = jnp.where(jnp.logical_and(below, square < TINY), FAR, y[0])
    return y


def point_at(y):
    square = sum(v * v for v in y)
    inverse = 1.0 / (1.0 + square)
    v = [(1.0 - square) * inverse, *(v * (2.0 * inverse) for v in y)]
    return list(zip(v[0::2], v[1::2]))


def sent(m):
    y = projected([e for v in m[0] for e in v])
    b = m[1]
    first, last = pivots(y)
    w = [*pick(first, b[1], b[0]), *pick(last, b[1], b[2])]
    scale = lax.rsqrt(sum(v * v for v in w))
    return y + projected([v * scale for v in w])


def received(load):
    v = [load(k) for k in range(VALUES)]
    a = point_at(v[:5])
    e, f = point_at(v[5:])
    first, last = pivots(v[:5])
    p, q = pick(first, a[1], a[0]), pick(last, a[1], a[2])
    top = pick(first, a[0], pick(last, a[2], a[1]))
    scale = -1.0 / (top[0] * top[0] + top[1] * top[1])
    g = mul(add(mul_conj(e, p), mul_conj(f, q)), top)
    g = (g[0] * scale, g[1] * scale)
    norm = lax.rsqrt(1.0 + g[0] * g[0] + g[1] * g[1])
    e, f, g = [(u[0] * norm, u[1] * norm) for u in (e, f, g)]
    return [a, [pick(first, g, e), pick(first, e, pick(last, f, g)), pick(last, g, f)]]


def send(store, m):
    for k, e in enumerate(sent(m)):
        store(k, e)


def at_rows(ref, rows_of_value):
    def store(k, v):
        ref[rows_of_value(k)] = v

    return store


def flat_rows(ref, size, first, count, stride=None):
    rows = lambda k: pl.ds(k * size + first, count, stride=stride)
    return lambda k: ref[rows(k), :], at_rows(ref, rows)


def rows_of(ref, first, count, stride=None, offset=0):
    rows = pl.ds(first, count, stride=stride)
    return lambda k: ref[offset + k, rows, :], at_rows(ref, lambda k: (offset + k, rows))


def gauge_kernel(n, links_ref, own_ref, near_ref, far_ref, edge_ref, g_ref, u_ref):
    lanes = links_ref.shape[-1]
    block = n * n
    near, far, edge = block + 2 * n - 1, 2 * n + 1, 2 * n - 1

    def raw(field, t, rows):
        part = lambda p, i, j: links_ref[field, p * 9 + i * 3 + j, pl.ds(t, n, stride=n), :]
        return [[(part(0, i, j), part(1, i, j)) for j in range(3)] for i in range(rows)]

    g = unit((n, lanes))
    for t in range(n):
        put(rows_of(g_ref, t * n, n)[1], completed(g))
        full = raw(0, t, 3)
        put(rows_of(u_ref, t * n, n)[1], product(g, full) if t else full[:2])
        step = raw(1, t, 3)
        g = product(g, step) if t else step[:2]
    put(rows_of(own_ref, block, n)[1], g)
    put(rows_of(own_ref, block + n, n - 1)[1], get(rows_of(g_ref, n, n - 1, n)[0]))
    send(flat_rows(near_ref, near, block, 2 * n - 1)[1], get(rows_of(own_ref, block, 2 * n - 1)[0]))
    last = lax.broadcasted_iota(jnp.int32, (8, lanes), 0) % n == n - 1
    for i in range(0, block, 8):
        after = where(last, unit((8, lanes), 3), get(rows_of(g_ref, i + 1, 8)[0], 3))
        w = product_dagger(get(rows_of(u_ref, i, 8)[0]), after)
        put(rows_of(own_ref, i, 8)[1], w)
        send(flat_rows(near_ref, near, i, 8)[1], w)
    for k in range(VALUES):
        far_ref[pl.ds(k * far, 2 * n), :] = near_ref[pl.ds(k * near, 2 * n), :]
        far_ref[pl.ds(k * far + 2 * n, 1), :] = near_ref[pl.ds(k * near + block + n, 1), :]
        edge_ref[pl.ds(k * edge, n), :] = near_ref[pl.ds(k * near, n, stride=n), :]
        edge_ref[pl.ds(k * edge + n, n - 1), :] = near_ref[pl.ds(k * near + block + n, n - 1), :]


def chain_kernel(n, own_ref, near_ref, far_ref, out_ref, late_ref, edge_ref, p_ref):
    lanes = own_ref.shape[-1]
    late, two, block = n + 2, 2 * n, n * n
    size = late * (n + 1)
    near, far = block + 2 * n - 1, 2 * n + 1

    def keep(first, count, m):
        put(flat_rows(out_ref, size, first, count)[1], m)
        send(flat_rows(late_ref, size, first, count)[1], m)

    def spread(p):
        p = completed(p)
        for k in range(3):
            put(rows_of(p_ref, k * n, n)[1], p)
        last = lax.broadcasted_iota(jnp.int32, (two, lanes), 0) % n == n - 1
        right = where(last, unit((two, lanes), 3), get(rows_of(p_ref, 1, two)[0], 3))
        return get(rows_of(p_ref, 0, two)[0]), right

    def first_of(p, count):
        return [[tuple(jnp.broadcast_to(e[0:1], (count, lanes)) for e in q) for q in row] for row in p]

    p = get(rows_of(own_ref, block, n)[0])
    p_next = received(flat_rows(near_ref, near, block, n)[0])
    pp = product(p, completed(p_next))
    hold = lambda first, count, m: put(flat_rows(out_ref, size, first, count)[1], m)
    hold(late * n, 1, first_of(p, 1))
    g = received(flat_rows(near_ref, near, block + n, n - 1)[0])
    hold(late * n + 1, n - 1, product(first_of(p, n - 1), completed(g)))
    hold(late * n + n, 1, first_of(pp, 1))
    g = received(flat_rows(far_ref, far, two, 1)[0])
    hold(late * n + n + 1, 1, product(first_of(pp, 1), completed(g)))
    left, right = spread(p)
    for i in range(0, block, 8):
        w = received(flat_rows(near_ref, near, i, 8)[0])
        keep(i, 8, product_dagger(product(left, completed(w)), right))
    left, right = spread(pp)
    w = received(flat_rows(far_ref, far, 0, two)[0])
    keep(block, two, product_dagger(product(left, completed(w)), right))
    send(flat_rows(late_ref, size, late * n, late)[1], get(flat_rows(out_ref, size, late * n, late)[0]))
    for k in range(VALUES):
        edge_ref[pl.ds(k * 2 * late, late), :] = late_ref[pl.ds(k * size, late, stride=n), :]
        edge_ref[pl.ds(k * 2 * late + late, late), :] = late_ref[pl.ds(k * size + late * n, late), :]


PAD = 8


def transports(n, times, a_ref, b_ref, c_ref, closing, store):
    lanes = a_ref.shape[-1]
    for ref, g in zip((a_ref, b_ref), closing):
        load, keep = rows_of(ref, PAD + n - 1, times, n)
        put(keep, completed(product_dagger(get(load), g)))
    x_of = lax.broadcasted_iota(jnp.int32, (8, lanes), 0) % n

    def window(k, i):
        own = lambda shift: get(rows_of(a_ref, PAD + i + shift, 8)[0], 3)
        after = lambda shift: get(rows_of(b_ref, PAD + i + shift, 8)[0], 3)
        if k == 0:
            return own(0)
        if k < n:
            return where(x_of < n - k, own(k), after(k - n))
        if k == n:
            return after(0)
        return where(x_of < n - 1, after(1), get(rows_of(c_ref, i, 8)[0], 3))

    for i in range(0, times * n, 8):
        s = window(0, i)[:2]
        for r in range(RMAX):
            if r:
                s = product(s, window(r, i))
            put(lambda c, v: store(r * 18 + c, i, v), completed(s))


def paired(pairs, at):
    sums = [None] * len(pairs)
    for c in range(18):
        for k, (p, q) in enumerate(pairs):
            e = at(c, p) * at(c, q)
            sums[k] = e if c == 0 else sums[k] + e
    return [jnp.sum(v, axis=1, keepdims=True) for v in sums]


def early_kernel(n, own_ref, near_ref, far_ref, s_ref, out_ref, a_ref, b_ref, c_ref, g_ref):
    lanes = own_ref.shape[-1]
    block = n * n
    near, edge = block + 2 * n - 1, 2 * n - 1
    for i in range(0, block, 8):
        put(rows_of(a_ref, PAD + i, 8)[1], completed(get(rows_of(own_ref, i, 8)[0])))
        put(rows_of(b_ref, PAD + i, 8)[1], completed(received(flat_rows(near_ref, near, i, 8)[0])))
    put(rows_of(c_ref, n - 1, n, n)[1], completed(received(flat_rows(far_ref, edge, 0, n)[0])))
    closing = []
    for k, load in enumerate((flat_rows(near_ref, near, block + n, n - 1), flat_rows(far_ref, edge, n, n - 1))):
        put(rows_of(g_ref, 0, 1, offset=12 * k)[1], unit((1, lanes)))
        put(rows_of(g_ref, 1, n - 1, offset=12 * k)[1], received(load[0]))
        closing.append(completed(get(rows_of(g_ref, 0, n, offset=12 * k)[0])))

    def store(c, i, v):
        s_ref[c, pl.ds(i, 8), :] = v

    transports(n, n, a_ref, b_ref, c_ref, closing, store)
    lane = lax.broadcasted_iota(jnp.int32, (8, lanes), 1)
    packed = jnp.zeros((8, lanes), jnp.float32)
    for r in range(RMAX):
        at = lambda c, t: s_ref[r * 18 + c, pl.ds(t * n, 8), :]
        for u, total in enumerate(paired([(0, 1), (0, 2)], at)):
            packed = jnp.where(lane == r * TMAX + u, total, packed)
    out_ref[...] = packed


def edge_kernel(n, far_ref, c_ref, g_ref):
    late = n + 2
    put(rows_of(c_ref, n - 1, late, n)[1], completed(received(flat_rows(far_ref, 2 * late, 0, late)[0])))
    put(rows_of(g_ref, 0, late)[1], completed(received(flat_rows(far_ref, 2 * late, late, late)[0])))


def late_kernel(n, own_ref, near_ref, c_ref, g_ref, early_ref, packed_ref, out_ref, a_ref, b_ref, s_ref):
    lanes = own_ref.shape[-1]
    late = n + 2
    size = late * (n + 1)
    for i in range(0, late * n, 8):
        put(rows_of(a_ref, PAD + i, 8)[1], completed(get(flat_rows(own_ref, size, i, 8)[0])))
        put(rows_of(b_ref, PAD + i, 8)[1], completed(received(flat_rows(near_ref, size, i, 8)[0])))
    closing = [
        completed(received(flat_rows(near_ref, size, late * n, late)[0])),
        get(rows_of(g_ref, 0, late)[0], 3),
    ]

    def store(c, i, v):
        s_ref[c, pl.ds(n + i, 8), :] = v

    transports(n, late, a_ref, b_ref, c_ref, closing, store)
    for c in range(RMAX * 18):
        s_ref[c, pl.ds(0, n), :] = early_ref[c, pl.ds(n * n - n, n), :]
    lane = lax.broadcasted_iota(jnp.int32, (8, lanes), 1)
    packed = [packed_ref[...], jnp.zeros((8, lanes), jnp.float32)]
    places = [(h, u) for u in range(1, TMAX + 1) for h in range(2) if (h, u) not in ((0, 1), (0, 2))]
    for r in range(RMAX):

        def at(c, t):
            if t < n - 1:
                return early_ref[r * 18 + c, pl.ds(t * n, 8), :]
            return s_ref[r * 18 + c, pl.ds((t - n + 1) * n, 8), :]

        for (h, u), total in zip(places, paired([(2 * h, 2 * h + u) for h, u in places], at)):
            packed[h] = jnp.where(lane == r * TMAX + u - 1, total, packed[h])
    for h in range(2):
        out_ref[pl.ds(8 * h, 8), :] = packed[h]


def last_kernel(n, scale, own_ref, other_ref, out_ref, v_ref):
    lanes = own_ref.shape[-1]
    total = (own_ref[...] + other_ref[...]) * scale
    for r in range(RMAX):
        v_ref[r] = pltpu.roll(total, lanes - r * TMAX, 1) if r else total
        for x in range(n):
            out_ref[r, x] = v_ref[r, pl.ds(x, n, stride=n), :][:, :TMAX]


def call(kernel, outs, scratch, *args, space=pltpu.VMEM):
    return pl.pallas_call(
        kernel,
        out_shape=[jax.ShapeDtypeStruct(s, jnp.float32) for s in outs],
        in_specs=[pl.BlockSpec(memory_space=space)] * len(args),
        out_specs=[pl.BlockSpec(memory_space=pltpu.VMEM)] * len(outs),
        scratch_shapes=[pltpu.VMEM(s, jnp.float32) if isinstance(s, tuple) else s for s in scratch],
        compiler_params=pltpu.CompilerParams(vmem_limit_bytes=8 * 2**20),
    )(*args)


def ahead(block, axis, distance):
    count = lax.axis_size(axis)
    return lax.ppermute(block, axis, [((i + distance) % count, i) for i in range(count)])


def local(link_x, link_t):
    n, lanes = link_x.shape[3], link_x.shape[5]
    if (n, link_x.shape[4], lanes) != (4, 4, 128):
        return plain(link_x, link_t)
    late, block = n + 2, n * n
    size, two = late * (n + 1), 2 * n
    flat = (18, block, lanes)
    own, near, far, edge = call(
        lambda *refs: gauge_kernel(n, *refs),
        [(12, block + two, lanes)] + [(VALUES * rows, lanes) for rows in (block + two - 1, two + 1, two - 1)],
        [(18, block + 8, lanes), (12, block, lanes)],
        jnp.stack([link_x.reshape(flat), link_t.reshape(flat)]),
    )
    near_t, far_t = ahead(near, "ta", 1), ahead(far, "ta", 2)
    near_x, edge_x = ahead(near, "gx", 1), ahead(edge, "gx", 2)
    own2, near2, edge2 = call(
        lambda *refs: chain_kernel(n, *refs),
        [(12 * size, lanes), (VALUES * size, lanes), (VALUES * 2 * late, lanes)],
        [(18, 3 * n, lanes)],
        own,
        near_t,
        far_t,
    )
    near2_x, edge2_x = ahead(near2, "gx", 1), ahead(edge2, "gx", 2)
    transport = (RMAX * 18, block, lanes)
    spaces = lambda rows: [(18, rows + 2 * PAD, lanes), (18, rows + 2 * PAD, lanes), (18, rows, lanes)]
    early, packed = call(
        lambda *refs: early_kernel(n, *refs),
        [transport, (8, lanes)],
        [*spaces(block), (24, 8, lanes)],
        own,
        near_x,
        edge_x,
    )
    after, close = call(
        lambda *refs: edge_kernel(n, *refs), [(18, late * n, lanes), (18, 8, lanes)], [], edge2_x
    )
    (packed,) = call(
        lambda *refs: late_kernel(n, *refs),
        [(16, lanes)],
        [*spaces(late * n)[:2], (RMAX * 18, (late + 1) * n, lanes)],
        own2,
        near2_x,
        after,
        close,
        early,
        packed,
    )
    count = lax.axis_size("gy")
    other = ahead(packed, "gy", 1) if count == 2 else lax.psum(packed, "gy") - packed
    scale = 1.0 / (3.0 * (lanes * count))
    (out,) = call(
        lambda *refs: last_kernel(n, scale, *refs),
        [(RMAX, n, n, TMAX)],
        [(RMAX, 4 * n, lanes)],
        packed,
        other,
    )
    return out.transpose(0, 3, 1, 2)


def shifted_2(block, axis, distance):
    devices = range(lax.axis_size(axis))
    route = [((i - distance) % len(devices), i) for i in devices]
    return lax.ppermute(block, axis, route)


def plain_times(left_mat, right_mat):
    real_rows = []
    imag_rows = []
    for i in range(3):
        real_cols = []
        imag_cols = []
        for k in range(3):
            real_sum = (
                left_mat[0, i, 0] * right_mat[0, 0, k] - left_mat[1, i, 0] * right_mat[1, 0, k]
            )
            imag_sum = (
                left_mat[0, i, 0] * right_mat[1, 0, k] + left_mat[1, i, 0] * right_mat[0, 0, k]
            )
            for j in range(1, 3):
                real_sum = (
                    real_sum
                    + left_mat[0, i, j] * right_mat[0, j, k]
                    - left_mat[1, i, j] * right_mat[1, j, k]
                )
                imag_sum = (
                    imag_sum
                    + left_mat[0, i, j] * right_mat[1, j, k]
                    + left_mat[1, i, j] * right_mat[0, j, k]
                )
            real_cols.append(real_sum)
            imag_cols.append(imag_sum)
        real_rows.append(jnp.stack(real_cols))
        imag_rows.append(jnp.stack(imag_cols))
    return jnp.stack([jnp.stack(real_rows), jnp.stack(imag_rows)])


def correlation(upper_half, lower_half):
    return jnp.sum(upper_half * lower_half, axis=(0, 1, 2, 5))


def next_x(field, along_dim):
    edge_cells = shifted_2(lax.slice_in_dim(field, 0, 1, axis=along_dim), "gx", -1)
    inner = lax.slice_in_dim(field, 1, field.shape[along_dim], axis=along_dim)
    return jnp.concatenate([inner, edge_cells], axis=along_dim)


def next_t(field):
    edge_cells = shifted_2(lax.slice_in_dim(field, 0, 1, axis=4), "ta", -1)
    inner = lax.slice_in_dim(field, 1, field.shape[4], axis=4)
    return jnp.concatenate([inner, edge_cells], axis=4)


def plain(link_x, link_t):
    all_rows = []
    temporal = [link_t]
    factor = link_t
    for _ in range(1, TMAX):
        factor = next_t(factor)
        temporal.append(plain_times(temporal[-1], factor))
    carried = jnp.stack(temporal)
    spatial = link_x
    factor_x = link_x
    for radius in range(RMAX):
        if radius > 0:
            factor_x = next_x(factor_x, 3)
            spatial = plain_times(spatial, factor_x)
        carried = next_x(carried, 4)
        shifted = spatial
        row_sums = []
        for extent in range(TMAX):
            shifted = next_t(shifted)
            upper_half = plain_times(spatial, carried[extent])
            lower_half = plain_times(temporal[extent], shifted)
            row_sums.append(correlation(upper_half, lower_half))
        all_rows.append(jnp.stack(row_sums))
    local_sums = jnp.stack(all_rows)
    totals = lax.psum(local_sums, "gy")
    return totals / (3.0 * (link_x.shape[5] * lax.axis_size("gy")))


def solution(mesh):
    return jax.shard_map(
        local,
        mesh=mesh,
        in_specs=(P(None, None, None, "gx", "ta", "gy"), P(None, None, None, "gx", "ta", "gy")),
        out_specs=P(None, None, "gx", "ta"),
        check_vma=False,
    )
```

```python
import jax
import jax.numpy as jnp
from jax import lax
from jax.experimental import pallas as pl
from jax.experimental.pallas import tpu as pltpu
from jax.sharding import PartitionSpec as P


RMAX = 6
TMAX = 6


def mul(a, b):
    return a[0] * b[0] - a[1] * b[1], a[0] * b[1] + a[1] * b[0]


def mul_conj(a, b):
    return a[0] * b[0] + a[1] * b[1], a[1] * b[0] - a[0] * b[1]


def add(a, b):
    return a[0] + b[0], a[1] + b[1]


def product(a, b):
    return [
        [add(add(mul(row[0], b[0][k]), mul(row[1], b[1][k])), mul(row[2], b[2][k])) for k in range(3)]
        for row in a
    ]


def product_dagger(a, b):
    return [
        [
            add(add(mul_conj(row[0], b[k][0]), mul_conj(row[1], b[k][1])), mul_conj(row[2], b[k][2]))
            for k in range(3)
        ]
        for row in a
    ]


def completed(a):
    last = []
    for k in range(3):
        i, j = (k + 1) % 3, (k + 2) % 3
        p, q = mul(a[0][i], a[1][j]), mul(a[0][j], a[1][i])
        last.append((p[0] - q[0], q[1] - p[1]))
    return [a[0], a[1], last]


def get(load, rows=2):
    return [[(load((3 * i + j) * 2), load((3 * i + j) * 2 + 1)) for j in range(3)] for i in range(rows)]


def put(store, a):
    for i, row in enumerate(a):
        for j in range(3):
            for k in range(2):
                store((3 * i + j) * 2 + k, row[j][k])


def where(mask, a, b):
    return [[tuple(jnp.where(mask, p, q) for p, q in zip(u, v)) for u, v in zip(r, s)] for r, s in zip(a, b)]


def unit(shape, rows=2):
    one, zero = jnp.ones(shape, jnp.float32), jnp.zeros(shape, jnp.float32)
    return [[(one if i == j else zero, zero) for j in range(3)] for i in range(rows)]


def pivots(y):
    sizes = [jnp.abs(v) for v in y]
    middle, end = jnp.maximum(sizes[1], sizes[2]), jnp.maximum(sizes[3], sizes[4])
    top = jnp.maximum(middle, end)
    other = jnp.logical_and(jnp.logical_and(top >= 0.35, top <= 1.5), sizes[0] <= 0.4)
    return jnp.logical_not(other), jnp.logical_and(other, end > middle)


def pick(mask, p, q):
    return tuple(jnp.where(mask, u, v) for u, v in zip(p, q))


VALUES = 8
TINY, FAR = 1e-30, 1e15


def projected(point):
    c, rest = point[0], point[1:]
    square = sum(v * v for v in rest)
    below = c < 0.0
    scale = jnp.where(below, 1.0 - c, 1.0) / jnp.where(below, jnp.maximum(square, TINY), 1.0 + c)
    y = [v * scale for v in rest]
    y[0] = jnp.where(jnp.logical_and(below, square < TINY), FAR, y[0])
    return y


def point_at(y):
    square = sum(v * v for v in y)
    inverse = 1.0 / (1.0 + square)
    v = [(1.0 - square) * inverse, *(v * (2.0 * inverse) for v in y)]
    return list(zip(v[0::2], v[1::2]))


def sent(m):
    y = projected([e for v in m[0] for e in v])
    b = m[1]
    first, last = pivots(y)
    w = [*pick(first, b[1], b[0]), *pick(last, b[1], b[2])]
    scale = lax.rsqrt(sum(v * v for v in w))
    return y + projected([v * scale for v in w])


def received(load):
    v = [load(k) for k in range(VALUES)]
    a = point_at(v[:5])
    e, f = point_at(v[5:])
    first, last = pivots(v[:5])
    p, q = pick(first, a[1], a[0]), pick(last, a[1], a[2])
    top = pick(first, a[0], pick(last, a[2], a[1]))
    scale = -1.0 / (top[0] * top[0] + top[1] * top[1])
    g = mul(add(mul_conj(e, p), mul_conj(f, q)), top)
    g = (g[0] * scale, g[1] * scale)
    norm = lax.rsqrt(1.0 + g[0] * g[0] + g[1] * g[1])
    e, f, g = [(u[0] * norm, u[1] * norm) for u in (e, f, g)]
    return [a, [pick(first, g, e), pick(first, e, pick(last, f, g)), pick(last, g, f)]]


def send(store, m):
    for k, e in enumerate(sent(m)):
        store(k, e)


def at_rows(ref, rows_of_value):
    def store(k, v):
        ref[rows_of_value(k)] = v

    return store


def flat_rows(ref, size, first, count, stride=None):
    rows = lambda k: pl.ds(k * size + first, count, stride=stride)
    return lambda k: ref[rows(k), :], at_rows(ref, rows)


def rows_of(ref, first, count, stride=None, offset=0):
    rows = pl.ds(first, count, stride=stride)
    return lambda k: ref[offset + k, rows, :], at_rows(ref, lambda k: (offset + k, rows))


def gauge_kernel(n, links_ref, own_ref, near_ref, far_ref, edge_ref, g_ref, u_ref):
    lanes = links_ref.shape[-1]
    block = n * n
    near, far, edge = block + 2 * n - 1, 2 * n + 1, 2 * n - 1

    def raw(field, t, rows):
        part = lambda p, i, j: links_ref[field, p * 9 + i * 3 + j, pl.ds(t, n, stride=n), :]
        return [[(part(0, i, j), part(1, i, j)) for j in range(3)] for i in range(rows)]

    g = unit((n, lanes))
    for t in range(n):
        put(rows_of(g_ref, t * n, n)[1], completed(g))
        full = raw(0, t, 3)
        put(rows_of(u_ref, t * n, n)[1], product(g, full) if t else full[:2])
        step = raw(1, t, 3)
        g = product(g, step) if t else step[:2]
    put(rows_of(own_ref, block, n)[1], g)
    put(rows_of(own_ref, block + n, n - 1)[1], get(rows_of(g_ref, n, n - 1, n)[0]))
    send(flat_rows(near_ref, near, block, 2 * n - 1)[1], get(rows_of(own_ref, block, 2 * n - 1)[0]))
    last = lax.broadcasted_iota(jnp.int32, (8, lanes), 0) % n == n - 1
    for i in range(0, block, 8):
        after = where(last, unit((8, lanes), 3), get(rows_of(g_ref, i + 1, 8)[0], 3))
        w = product_dagger(get(rows_of(u_ref, i, 8)[0]), after)
        put(rows_of(own_ref, i, 8)[1], w)
        send(flat_rows(near_ref, near, i, 8)[1], w)
    for k in range(VALUES):
        far_ref[pl.ds(k * far, 2 * n), :] = near_ref[pl.ds(k * near, 2 * n), :]
        far_ref[pl.ds(k * far + 2 * n, 1), :] = near_ref[pl.ds(k * near + block + n, 1), :]
        edge_ref[pl.ds(k * edge, n), :] = near_ref[pl.ds(k * near, n, stride=n), :]
        edge_ref[pl.ds(k * edge + n, n - 1), :] = near_ref[pl.ds(k * near + block + n, n - 1), :]


def chain_kernel(n, own_ref, near_ref, far_ref, out_ref, late_ref, edge_ref, p_ref):
    lanes = own_ref.shape[-1]
    late, two, block = n + 2, 2 * n, n * n
    size = late * (n + 1)
    near, far = block + 2 * n - 1, 2 * n + 1

    def keep(first, count, m):
        put(flat_rows(out_ref, size, first, count)[1], m)
        send(flat_rows(late_ref, size, first, count)[1], m)

    def spread(p):
        p = completed(p)
        for k in range(3):
            put(rows_of(p_ref, k * n, n)[1], p)
        last = lax.broadcasted_iota(jnp.int32, (two, lanes), 0) % n == n - 1
        right = where(last, unit((two, lanes), 3), get(rows_of(p_ref, 1, two)[0], 3))
        return get(rows_of(p_ref, 0, two)[0]), right

    def first_of(p, count):
        return [[tuple(jnp.broadcast_to(e[0:1], (count, lanes)) for e in q) for q in row] for row in p]

    p = get(rows_of(own_ref, block, n)[0])
    p_next = received(flat_rows(near_ref, near, block, n)[0])
    pp = product(p, completed(p_next))
    hold = lambda first, count, m: put(flat_rows(out_ref, size, first, count)[1], m)
    hold(late * n, 1, first_of(p, 1))
    g = received(flat_rows(near_ref, near, block + n, n - 1)[0])
    hold(late * n + 1, n - 1, product(first_of(p, n - 1), completed(g)))
    hold(late * n + n, 1, first_of(pp, 1))
    g = received(flat_rows(far_ref, far, two, 1)[0])
    hold(late * n + n + 1, 1, product(first_of(pp, 1), completed(g)))
    left, right = spread(p)
    for i in range(0, block, 8):
        w = received(flat_rows(near_ref, near, i, 8)[0])
        keep(i, 8, product_dagger(product(left, completed(w)), right))
    left, right = spread(pp)
    w = received(flat_rows(far_ref, far, 0, two)[0])
    keep(block, two, product_dagger(product(left, completed(w)), right))
    send(flat_rows(late_ref, size, late * n, late)[1], get(flat_rows(out_ref, size, late * n, late)[0]))
    for k in range(VALUES):
        edge_ref[pl.ds(k * 2 * late, late), :] = late_ref[pl.ds(k * size, late, stride=n), :]
        edge_ref[pl.ds(k * 2 * late + late, late), :] = late_ref[pl.ds(k * size + late * n, late), :]


PAD = 8


def transports(n, times, a_ref, b_ref, c_ref, closing, store):
    lanes = a_ref.shape[-1]
    for ref, g in zip((a_ref, b_ref), closing):
        load, keep = rows_of(ref, PAD + n - 1, times, n)
        put(keep, completed(product_dagger(get(load), completed(g))))
    x_of = lax.broadcasted_iota(jnp.int32, (8, lanes), 0) % n

    def window(k, i):
        own = lambda shift: get(rows_of(a_ref, PAD + i + shift, 8)[0], 3)
        after = lambda shift: get(rows_of(b_ref, PAD + i + shift, 8)[0], 3)
        if k == 0:
            return own(0)
        if k < n:
            return where(x_of < n - k, own(k), after(k - n))
        if k == n:
            return after(0)
        return where(x_of < n - 1, after(1), get(rows_of(c_ref, i, 8)[0], 3))

    for i in range(0, times * n, 8):
        s = window(0, i)[:2]
        for r in range(RMAX):
            if r:
                s = product(s, window(r, i))
            put(lambda c, v: store(r * 18 + c, i, v), completed(s))


def paired(pairs, at):
    sums = [None] * len(pairs)
    for c in range(18):
        for k, (p, q) in enumerate(pairs):
            e = at(c, p) * at(c, q)
            sums[k] = e if c == 0 else sums[k] + e
    return [jnp.sum(v, axis=1, keepdims=True) for v in sums]


def early_kernel(n, own_ref, near_ref, far_ref, s_ref, out_ref, a_ref, b_ref, c_ref, g_ref):
    lanes = own_ref.shape[-1]
    block = n * n
    near, edge = block + 2 * n - 1, 2 * n - 1
    for i in range(0, block, 8):
        put(rows_of(a_ref, PAD + i, 8)[1], completed(get(rows_of(own_ref, i, 8)[0])))
        put(rows_of(b_ref, PAD + i, 8)[1], completed(received(flat_rows(near_ref, near, i, 8)[0])))
    put(rows_of(c_ref, n - 1, n, n)[1], completed(received(flat_rows(far_ref, edge, 0, n)[0])))
    closing = []
    for k, load in enumerate((flat_rows(near_ref, near, block + n, n - 1), flat_rows(far_ref, edge, n, n - 1))):
        put(rows_of(g_ref, 0, 1, offset=12 * k)[1], unit((1, lanes)))
        put(rows_of(g_ref, 1, n - 1, offset=12 * k)[1], received(load[0]))
        closing.append(get(rows_of(g_ref, 0, n, offset=12 * k)[0]))

    def store(c, i, v):
        s_ref[c, pl.ds(i, 8), :] = v

    transports(n, n, a_ref, b_ref, c_ref, closing, store)
    lane = lax.broadcasted_iota(jnp.int32, (8, lanes), 1)
    packed = jnp.zeros((8, lanes), jnp.float32)
    for r in range(RMAX):
        at = lambda c, t: s_ref[r * 18 + c, pl.ds(t * n, 8), :]
        for u, total in enumerate(paired([(0, 1), (0, 2)], at)):
            packed = jnp.where(lane == r * TMAX + u, total, packed)
    out_ref[...] = packed


def late_kernel(n, own_ref, near_ref, far_ref, early_ref, packed_ref, out_ref, a_ref, b_ref, c_ref, s_ref):
    lanes = own_ref.shape[-1]
    late = n + 2
    size = late * (n + 1)
    for i in range(0, late * n, 8):
        put(rows_of(a_ref, PAD + i, 8)[1], completed(get(flat_rows(own_ref, size, i, 8)[0])))
        put(rows_of(b_ref, PAD + i, 8)[1], completed(received(flat_rows(near_ref, size, i, 8)[0])))
    put(rows_of(c_ref, n - 1, late, n)[1], completed(received(flat_rows(far_ref, 2 * late, 0, late)[0])))
    closing = [
        received(flat_rows(near_ref, size, late * n, late)[0]),
        received(flat_rows(far_ref, 2 * late, late, late)[0]),
    ]

    def store(c, i, v):
        s_ref[c, pl.ds(n + i, 8), :] = v

    transports(n, late, a_ref, b_ref, c_ref, closing, store)
    for c in range(RMAX * 18):
        s_ref[c, pl.ds(0, n), :] = early_ref[c, pl.ds(n * n - n, n), :]
    lane = lax.broadcasted_iota(jnp.int32, (8, lanes), 1)
    packed = [packed_ref[...], jnp.zeros((8, lanes), jnp.float32)]
    places = [(h, u) for u in range(1, TMAX + 1) for h in range(2) if (h, u) not in ((0, 1), (0, 2))]
    for r in range(RMAX):

        def at(c, t):
            if t < n - 1:
                return early_ref[r * 18 + c, pl.ds(t * n, 8), :]
            return s_ref[r * 18 + c, pl.ds((t - n + 1) * n, 8), :]

        for (h, u), total in zip(places, paired([(2 * h, 2 * h + u) for h, u in places], at)):
            packed[h] = jnp.where(lane == r * TMAX + u - 1, total, packed[h])
    for h in range(2):
        out_ref[pl.ds(8 * h, 8), :] = packed[h]


def last_kernel(n, scale, own_ref, other_ref, out_ref, v_ref):
    lanes = own_ref.shape[-1]
    total = (own_ref[...] + other_ref[...]) * scale
    for r in range(RMAX):
        v_ref[r] = pltpu.roll(total, lanes - r * TMAX, 1) if r else total
        for x in range(n):
            out_ref[r, x] = v_ref[r, pl.ds(x, n, stride=n), :][:, :TMAX]


def call(kernel, outs, scratch, *args, space=pltpu.VMEM, fuse=False):
    return pl.pallas_call(
        kernel,
        out_shape=[jax.ShapeDtypeStruct(s, jnp.float32) for s in outs],
        in_specs=[pl.BlockSpec(memory_space=space)] * len(args),
        out_specs=[pl.BlockSpec(memory_space=pltpu.VMEM)] * len(outs),
        scratch_shapes=[pltpu.VMEM(s, jnp.float32) if isinstance(s, tuple) else s for s in scratch],
        compiler_params=pltpu.CompilerParams(vmem_limit_bytes=8 * 2**20, allow_input_fusion=[True] * len(args) if fuse else None),
    )(*args)


def ahead(block, axis, distance):
    count = lax.axis_size(axis)
    return lax.ppermute(block, axis, [((i + distance) % count, i) for i in range(count)])


def local(link_x, link_t):
    n, lanes = link_x.shape[3], link_x.shape[5]
    if (n, link_x.shape[4], lanes) != (4, 4, 128):
        return plain(link_x, link_t)
    late, block = n + 2, n * n
    size, two = late * (n + 1), 2 * n
    flat = (18, block, lanes)
    own, near, far, edge = call(
        lambda *refs: gauge_kernel(n, *refs),
        [(12, block + two, lanes)] + [(VALUES * rows, lanes) for rows in (block + two - 1, two + 1, two - 1)],
        [(18, block + 8, lanes), (12, block, lanes)],
        jnp.stack([link_x.reshape(flat), link_t.reshape(flat)]),
        fuse=True,
    )
    near_t, far_t = ahead(near, "ta", 1), ahead(far, "ta", 2)
    near_x, edge_x = ahead(near, "gx", 1), ahead(edge, "gx", 2)
    own2, near2, edge2 = call(
        lambda *refs: chain_kernel(n, *refs),
        [(12 * size, lanes), (VALUES * size, lanes), (VALUES * 2 * late, lanes)],
        [(18, 3 * n, lanes)],
        own,
        near_t,
        far_t,
    )
    near2_x, edge2_x = ahead(near2, "gx", 1), ahead(edge2, "gx", 2)
    transport = (RMAX * 18, block, lanes)
    spaces = lambda rows: [(18, rows + 2 * PAD, lanes), (18, rows + 2 * PAD, lanes), (18, rows, lanes)]
    early, packed = call(
        lambda *refs: early_kernel(n, *refs),
        [transport, (8, lanes)],
        [*spaces(block), (24, 8, lanes)],
        own,
        near_x,
        edge_x,
    )
    (packed,) = call(
        lambda *refs: late_kernel(n, *refs),
        [(16, lanes)],
        [*spaces(late * n), (RMAX * 18, (late + 1) * n, lanes)],
        own2,
        near2_x,
        edge2_x,
        early,
        packed,
    )
    count = lax.axis_size("gy")
    other = ahead(packed, "gy", 1) if count == 2 else lax.psum(packed, "gy") - packed
    scale = 1.0 / (3.0 * (lanes * count))
    (out,) = call(
        lambda *refs: last_kernel(n, scale, *refs),
        [(RMAX, n, n, TMAX)],
        [(RMAX, 4 * n, lanes)],
        packed,
        other,
    )
    return out.transpose(0, 3, 1, 2)


def shifted_2(block, axis, distance):
    devices = range(lax.axis_size(axis))
    route = [((i - distance) % len(devices), i) for i in devices]
    return lax.ppermute(block, axis, route)


def plain_times(left_mat, right_mat):
    real_rows = []
    imag_rows = []
    for i in range(3):
        real_cols = []
        imag_cols = []
        for k in range(3):
            real_sum = (
                left_mat[0, i, 0] * right_mat[0, 0, k] - left_mat[1, i, 0] * right_mat[1, 0, k]
            )
            imag_sum = (
                left_mat[0, i, 0] * right_mat[1, 0, k] + left_mat[1, i, 0] * right_mat[0, 0, k]
            )
            for j in range(1, 3):
                real_sum = (
                    real_sum
                    + left_mat[0, i, j] * right_mat[0, j, k]
                    - left_mat[1, i, j] * right_mat[1, j, k]
                )
                imag_sum = (
                    imag_sum
                    + left_mat[0, i, j] * right_mat[1, j, k]
                    + left_mat[1, i, j] * right_mat[0, j, k]
                )
            real_cols.append(real_sum)
            imag_cols.append(imag_sum)
        real_rows.append(jnp.stack(real_cols))
        imag_rows.append(jnp.stack(imag_cols))
    return jnp.stack([jnp.stack(real_rows), jnp.stack(imag_rows)])


def correlation(upper_half, lower_half):
    return jnp.sum(upper_half * lower_half, axis=(0, 1, 2, 5))


def next_x(field, along_dim):
    edge_cells = shifted_2(lax.slice_in_dim(field, 0, 1, axis=along_dim), "gx", -1)
    inner = lax.slice_in_dim(field, 1, field.shape[along_dim], axis=along_dim)
    return jnp.concatenate([inner, edge_cells], axis=along_dim)


def next_t(field):
    edge_cells = shifted_2(lax.slice_in_dim(field, 0, 1, axis=4), "ta", -1)
    inner = lax.slice_in_dim(field, 1, field.shape[4], axis=4)
    return jnp.concatenate([inner, edge_cells], axis=4)


def plain(link_x, link_t):
    all_rows = []
    temporal = [link_t]
    factor = link_t
    for _ in range(1, TMAX):
        factor = next_t(factor)
        temporal.append(plain_times(temporal[-1], factor))
    carried = jnp.stack(temporal)
    spatial = link_x
    factor_x = link_x
    for radius in range(RMAX):
        if radius > 0:
            factor_x = next_x(factor_x, 3)
            spatial = plain_times(spatial, factor_x)
        carried = next_x(carried, 4)
        shifted = spatial
        row_sums = []
        for extent in range(TMAX):
            shifted = next_t(shifted)
            upper_half = plain_times(spatial, carried[extent])
            lower_half = plain_times(temporal[extent], shifted)
            row_sums.append(correlation(upper_half, lower_half))
        all_rows.append(jnp.stack(row_sums))
    local_sums = jnp.stack(all_rows)
    totals = lax.psum(local_sums, "gy")
    return totals / (3.0 * (link_x.shape[5] * lax.axis_size("gy")))


def solution(mesh):
    return jax.shard_map(
        local,
        mesh=mesh,
        in_specs=(P(None, None, None, "gx", "ta", "gy"), P(None, None, None, "gx", "ta", "gy")),
        out_specs=P(None, None, "gx", "ta"),
        check_vma=False,
    )
```

```python
import jax
import jax.numpy as jnp
from jax import lax
from jax.experimental import pallas as pl
from jax.experimental.pallas import tpu as pltpu
from jax.sharding import PartitionSpec as P


RMAX = 6
TMAX = 6


def mul(a, b):
    return a[0] * b[0] - a[1] * b[1], a[0] * b[1] + a[1] * b[0]


def mul_conj(a, b):
    return a[0] * b[0] + a[1] * b[1], a[1] * b[0] - a[0] * b[1]


def add(a, b):
    return a[0] + b[0], a[1] + b[1]


def product(a, b):
    return [
        [add(add(mul(row[0], b[0][k]), mul(row[1], b[1][k])), mul(row[2], b[2][k])) for k in range(3)]
        for row in a
    ]


def product_dagger(a, b):
    return [
        [
            add(add(mul_conj(row[0], b[k][0]), mul_conj(row[1], b[k][1])), mul_conj(row[2], b[k][2]))
            for k in range(3)
        ]
        for row in a
    ]


def completed(a):
    last = []
    for k in range(3):
        i, j = (k + 1) % 3, (k + 2) % 3
        p, q = mul(a[0][i], a[1][j]), mul(a[0][j], a[1][i])
        last.append((p[0] - q[0], q[1] - p[1]))
    return [a[0], a[1], last]


def get(load, rows=2):
    return [[(load((3 * i + j) * 2), load((3 * i + j) * 2 + 1)) for j in range(3)] for i in range(rows)]


def put(store, a):
    for i, row in enumerate(a):
        for j in range(3):
            for k in range(2):
                store((3 * i + j) * 2 + k, row[j][k])


def where(mask, a, b):
    return [[tuple(jnp.where(mask, p, q) for p, q in zip(u, v)) for u, v in zip(r, s)] for r, s in zip(a, b)]


def unit(shape, rows=2):
    one, zero = jnp.ones(shape, jnp.float32), jnp.zeros(shape, jnp.float32)
    return [[(one if i == j else zero, zero) for j in range(3)] for i in range(rows)]


def pivots(y):
    sizes = [jnp.abs(v) for v in y]
    middle, end = jnp.maximum(sizes[1], sizes[2]), jnp.maximum(sizes[3], sizes[4])
    top = jnp.maximum(middle, end)
    other = jnp.logical_and(jnp.logical_and(top >= 0.35, top <= 1.5), sizes[0] <= 0.4)
    return jnp.logical_not(other), jnp.logical_and(other, end > middle)


def pick(mask, p, q):
    return tuple(jnp.where(mask, u, v) for u, v in zip(p, q))


VALUES = 8
TINY, FAR = 1e-30, 1e15


def projected(point):
    c, rest = point[0], point[1:]
    square = sum(v * v for v in rest)
    below = c < 0.0
    scale = jnp.where(below, 1.0 - c, 1.0) / jnp.where(below, jnp.maximum(square, TINY), 1.0 + c)
    y = [v * scale for v in rest]
    y[0] = jnp.where(jnp.logical_and(below, square < TINY), FAR, y[0])
    return y


def point_at(y):
    square = sum(v * v for v in y)
    inverse = 1.0 / (1.0 + square)
    v = [(1.0 - square) * inverse, *(v * (2.0 * inverse) for v in y)]
    return list(zip(v[0::2], v[1::2]))


def sent(m):
    y = projected([e for v in m[0] for e in v])
    b = m[1]
    first, last = pivots(y)
    w = [*pick(first, b[1], b[0]), *pick(last, b[1], b[2])]
    scale = lax.rsqrt(sum(v * v for v in w))
    return y + projected([v * scale for v in w])


def received(load):
    v = [load(k) for k in range(VALUES)]
    a = point_at(v[:5])
    e, f = point_at(v[5:])
    first, last = pivots(v[:5])
    p, q = pick(first, a[1], a[0]), pick(last, a[1], a[2])
    top = pick(first, a[0], pick(last, a[2], a[1]))
    scale = -1.0 / (top[0] * top[0] + top[1] * top[1])
    g = mul(add(mul_conj(e, p), mul_conj(f, q)), top)
    g = (g[0] * scale, g[1] * scale)
    norm = lax.rsqrt(1.0 + g[0] * g[0] + g[1] * g[1])
    e, f, g = [(u[0] * norm, u[1] * norm) for u in (e, f, g)]
    return [a, [pick(first, g, e), pick(first, e, pick(last, f, g)), pick(last, g, f)]]


def send(store, m):
    for k, e in enumerate(sent(m)):
        store(k, e)


def at_rows(ref, rows_of_value):
    def store(k, v):
        ref[rows_of_value(k)] = v

    return store


def flat_rows(ref, size, first, count, stride=None):
    rows = lambda k: pl.ds(k * size + first, count, stride=stride)
    return lambda k: ref[rows(k), :], at_rows(ref, rows)


def rows_of(ref, first, count, stride=None, offset=0):
    rows = pl.ds(first, count, stride=stride)
    return lambda k: ref[offset + k, rows, :], at_rows(ref, lambda k: (offset + k, rows))


def gauge_kernel(n, links_ref, own_ref, near_ref, far_ref, edge_ref, g_ref, u_ref):
    lanes = links_ref.shape[-1]
    block = n * n
    near, far, edge = block + 2 * n - 1, 2 * n + 1, 2 * n - 1

    def raw(field, t, rows):
        part = lambda p, i, j: links_ref[field, p * 9 + i * 3 + j, pl.ds(t, n, stride=n), :]
        return [[(part(0, i, j), part(1, i, j)) for j in range(3)] for i in range(rows)]

    g = unit((n, lanes))
    for t in range(n):
        put(rows_of(g_ref, t * n, n)[1], completed(g))
        full = raw(0, t, 3)
        put(rows_of(u_ref, t * n, n)[1], product(g, full) if t else full[:2])
        step = raw(1, t, 3)
        g = product(g, step) if t else step[:2]
    put(rows_of(own_ref, block, n)[1], g)
    put(rows_of(own_ref, block + n, n - 1)[1], get(rows_of(g_ref, n, n - 1, n)[0]))
    send(flat_rows(near_ref, near, block, 2 * n - 1)[1], get(rows_of(own_ref, block, 2 * n - 1)[0]))
    last = lax.broadcasted_iota(jnp.int32, (8, lanes), 0) % n == n - 1
    for i in range(0, block, 8):
        after = where(last, unit((8, lanes), 3), get(rows_of(g_ref, i + 1, 8)[0], 3))
        w = product_dagger(get(rows_of(u_ref, i, 8)[0]), after)
        put(rows_of(own_ref, i, 8)[1], w)
        send(flat_rows(near_ref, near, i, 8)[1], w)
    for k in range(VALUES):
        far_ref[pl.ds(k * far, 2 * n), :] = near_ref[pl.ds(k * near, 2 * n), :]
        far_ref[pl.ds(k * far + 2 * n, 1), :] = near_ref[pl.ds(k * near + block + n, 1), :]
        edge_ref[pl.ds(k * edge, n), :] = near_ref[pl.ds(k * near, n, stride=n), :]
        edge_ref[pl.ds(k * edge + n, n - 1), :] = near_ref[pl.ds(k * near + block + n, n - 1), :]


def chain_kernel(n, own_ref, near_ref, far_ref, out_ref, late_ref, edge_ref, p_ref):
    lanes = own_ref.shape[-1]
    late, two, block = n + 2, 2 * n, n * n
    size = late * (n + 1)
    near, far = block + 2 * n - 1, 2 * n + 1

    def keep(first, count, m):
        put(flat_rows(out_ref, size, first, count)[1], m)
        send(flat_rows(late_ref, size, first, count)[1], m)

    def spread(p):
        p = completed(p)
        for k in range(3):
            put(rows_of(p_ref, k * n, n)[1], p)
        last = lax.broadcasted_iota(jnp.int32, (two, lanes), 0) % n == n - 1
        right = where(last, unit((two, lanes), 3), get(rows_of(p_ref, 1, two)[0], 3))
        return get(rows_of(p_ref, 0, two)[0]), right

    def first_of(p, count):
        return [[tuple(jnp.broadcast_to(e[0:1], (count, lanes)) for e in q) for q in row] for row in p]

    p = get(rows_of(own_ref, block, n)[0])
    p_next = received(flat_rows(near_ref, near, block, n)[0])
    pp = product(p, completed(p_next))
    hold = lambda first, count, m: put(flat_rows(out_ref, size, first, count)[1], m)
    hold(late * n, 1, first_of(p, 1))
    g = received(flat_rows(near_ref, near, block + n, n - 1)[0])
    hold(late * n + 1, n - 1, product(first_of(p, n - 1), completed(g)))
    hold(late * n + n, 1, first_of(pp, 1))
    g = received(flat_rows(far_ref, far, two, 1)[0])
    hold(late * n + n + 1, 1, product(first_of(pp, 1), completed(g)))
    left, right = spread(p)
    for i in range(0, block, 8):
        w = received(flat_rows(near_ref, near, i, 8)[0])
        keep(i, 8, product_dagger(product(left, completed(w)), right))
    left, right = spread(pp)
    w = received(flat_rows(far_ref, far, 0, two)[0])
    keep(block, two, product_dagger(product(left, completed(w)), right))
    send(flat_rows(late_ref, size, late * n, late)[1], get(flat_rows(out_ref, size, late * n, late)[0]))
    for k in range(VALUES):
        edge_ref[pl.ds(k * 2 * late, late), :] = late_ref[pl.ds(k * size, late, stride=n), :]
        edge_ref[pl.ds(k * 2 * late + late, late), :] = late_ref[pl.ds(k * size + late * n, late), :]


PAD = 8


def transports(n, times, a_ref, b_ref, c_ref, closing, store):
    lanes = a_ref.shape[-1]
    for ref, g in zip((a_ref, b_ref), closing):
        load, keep = rows_of(ref, PAD + n - 1, times, n)
        put(keep, completed(product_dagger(get(load), g)))
    x_of = lax.broadcasted_iota(jnp.int32, (8, lanes), 0) % n

    def window(k, i):
        own = lambda shift: get(rows_of(a_ref, PAD + i + shift, 8)[0], 3)
        after = lambda shift: get(rows_of(b_ref, PAD + i + shift, 8)[0], 3)
        if k == 0:
            return own(0)
        if k < n:
            return where(x_of < n - k, own(k), after(k - n))
        if k == n:
            return after(0)
        return where(x_of < n - 1, after(1), get(rows_of(c_ref, i, 8)[0], 3))

    for i in range(0, times * n, 8):
        s = window(0, i)[:2]
        for r in range(RMAX):
            if r:
                s = product(s, window(r, i))
            put(lambda c, v: store(r * 18 + c, i, v), completed(s))


def paired(pairs, at):
    sums = [None] * len(pairs)
    for c in range(18):
        for k, (p, q) in enumerate(pairs):
            e = at(c, p) * at(c, q)
            sums[k] = e if c == 0 else sums[k] + e
    return [jnp.sum(v, axis=1, keepdims=True) for v in sums]


def early_kernel(n, own_ref, near_ref, far_ref, s_ref, out_ref, a_ref, b_ref, c_ref, g_ref):
    lanes = own_ref.shape[-1]
    block = n * n
    near, edge = block + 2 * n - 1, 2 * n - 1
    for i in range(0, block, 8):
        put(rows_of(a_ref, PAD + i, 8)[1], completed(get(rows_of(own_ref, i, 8)[0])))
        put(rows_of(b_ref, PAD + i, 8)[1], completed(received(flat_rows(near_ref, near, i, 8)[0])))
    put(rows_of(c_ref, n - 1, n, n)[1], completed(received(flat_rows(far_ref, edge, 0, n)[0])))
    closing = []
    for k, load in enumerate((flat_rows(near_ref, near, block + n, n - 1), flat_rows(far_ref, edge, n, n - 1))):
        put(rows_of(g_ref, 0, 1, offset=12 * k)[1], unit((1, lanes)))
        put(rows_of(g_ref, 1, n - 1, offset=12 * k)[1], received(load[0]))
        closing.append(completed(get(rows_of(g_ref, 0, n, offset=12 * k)[0])))

    def store(c, i, v):
        s_ref[c, pl.ds(i, 8), :] = v

    transports(n, n, a_ref, b_ref, c_ref, closing, store)
    lane = lax.broadcasted_iota(jnp.int32, (8, lanes), 1)
    packed = jnp.zeros((8, lanes), jnp.float32)
    for r in range(RMAX):
        at = lambda c, t: s_ref[r * 18 + c, pl.ds(t * n, 8), :]
        for u, total in enumerate(paired([(0, 1), (0, 2)], at)):
            packed = jnp.where(lane == r * TMAX + u, total, packed)
    out_ref[...] = packed


def edge_kernel(n, far_ref, c_ref, g_ref):
    late = n + 2
    put(rows_of(c_ref, n - 1, late, n)[1], completed(received(flat_rows(far_ref, 2 * late, 0, late)[0])))
    put(rows_of(g_ref, 0, late)[1], completed(received(flat_rows(far_ref, 2 * late, late, late)[0])))


def late_kernel(n, own_ref, near_ref, c_ref, g_ref, early_ref, packed_ref, out_ref, a_ref, b_ref, s_ref):
    lanes = own_ref.shape[-1]
    late = n + 2
    size = late * (n + 1)
    for i in range(0, late * n, 8):
        put(rows_of(a_ref, PAD + i, 8)[1], completed(get(flat_rows(own_ref, size, i, 8)[0])))
        put(rows_of(b_ref, PAD + i, 8)[1], completed(received(flat_rows(near_ref, size, i, 8)[0])))
    closing = [
        completed(received(flat_rows(near_ref, size, late * n, late)[0])),
        get(rows_of(g_ref, 0, late)[0], 3),
    ]

    def store(c, i, v):
        s_ref[c, pl.ds(n + i, 8), :] = v

    transports(n, late, a_ref, b_ref, c_ref, closing, store)
    for c in range(RMAX * 18):
        s_ref[c, pl.ds(0, n), :] = early_ref[c, pl.ds(n * n - n, n), :]
    lane = lax.broadcasted_iota(jnp.int32, (8, lanes), 1)
    packed = [packed_ref[...], jnp.zeros((8, lanes), jnp.float32)]
    places = [(h, u) for u in range(1, TMAX + 1) for h in range(2) if (h, u) not in ((0, 1), (0, 2))]
    for r in range(RMAX):

        def at(c, t):
            if t < n - 1:
                return early_ref[r * 18 + c, pl.ds(t * n, 8), :]
            return s_ref[r * 18 + c, pl.ds((t - n + 1) * n, 8), :]

        for (h, u), total in zip(places, paired([(2 * h, 2 * h + u) for h, u in places], at)):
            packed[h] = jnp.where(lane == r * TMAX + u - 1, total, packed[h])
    for h in range(2):
        out_ref[pl.ds(8 * h, 8), :] = packed[h]


def last_kernel(n, scale, own_ref, other_ref, out_ref, v_ref):
    lanes = own_ref.shape[-1]
    total = (own_ref[...] + other_ref[...]) * scale
    for r in range(RMAX):
        v_ref[r] = pltpu.roll(total, lanes - r * TMAX, 1) if r else total
        for x in range(n):
            out_ref[r, x] = v_ref[r, pl.ds(x, n, stride=n), :][:, :TMAX]


def call(kernel, outs, scratch, *args, space=pltpu.VMEM, fuse=False):
    return pl.pallas_call(
        kernel,
        out_shape=[jax.ShapeDtypeStruct(s, jnp.float32) for s in outs],
        in_specs=[pl.BlockSpec(memory_space=space)] * len(args),
        out_specs=[pl.BlockSpec(memory_space=pltpu.VMEM)] * len(outs),
        scratch_shapes=[pltpu.VMEM(s, jnp.float32) if isinstance(s, tuple) else s for s in scratch],
        compiler_params=pltpu.CompilerParams(vmem_limit_bytes=8 * 2**20, allow_input_fusion=[True] * len(args) if fuse else None),
    )(*args)


def ahead(block, axis, distance):
    count = lax.axis_size(axis)
    return lax.ppermute(block, axis, [((i + distance) % count, i) for i in range(count)])


def local(link_x, link_t):
    n, lanes = link_x.shape[3], link_x.shape[5]
    if (n, link_x.shape[4], lanes) != (4, 4, 128):
        return plain(link_x, link_t)
    late, block = n + 2, n * n
    size, two = late * (n + 1), 2 * n
    flat = (18, block, lanes)
    own, near, far, edge = call(
        lambda *refs: gauge_kernel(n, *refs),
        [(12, block + two, lanes)] + [(VALUES * rows, lanes) for rows in (block + two - 1, two + 1, two - 1)],
        [(18, block + 8, lanes), (12, block, lanes)],
        jnp.stack([link_x.reshape(flat), link_t.reshape(flat)]),
        fuse=True,
    )
    near_t, far_t = ahead(near, "ta", 1), ahead(far, "ta", 2)
    near_x, edge_x = ahead(near, "gx", 1), ahead(edge, "gx", 2)
    own2, near2, edge2 = call(
        lambda *refs: chain_kernel(n, *refs),
        [(12 * size, lanes), (VALUES * size, lanes), (VALUES * 2 * late, lanes)],
        [(18, 3 * n, lanes)],
        own,
        near_t,
        far_t,
    )
    near2_x, edge2_x = ahead(near2, "gx", 1), ahead(edge2, "gx", 2)
    transport = (RMAX * 18, block, lanes)
    spaces = lambda rows: [(18, rows + 2 * PAD, lanes), (18, rows + 2 * PAD, lanes), (18, rows, lanes)]
    early, packed = call(
        lambda *refs: early_kernel(n, *refs),
        [transport, (8, lanes)],
        [*spaces(block), (24, 8, lanes)],
        own,
        near_x,
        edge_x,
    )
    after, close = call(
        lambda *refs: edge_kernel(n, *refs), [(18, late * n, lanes), (18, 8, lanes)], [], edge2_x
    )
    (packed,) = call(
        lambda *refs: late_kernel(n, *refs),
        [(16, lanes)],
        [*spaces(late * n)[:2], (RMAX * 18, (late + 1) * n, lanes)],
        own2,
        near2_x,
        after,
        close,
        early,
        packed,
    )
    count = lax.axis_size("gy")
    other = ahead(packed, "gy", 1) if count == 2 else lax.psum(packed, "gy") - packed
    scale = 1.0 / (3.0 * (lanes * count))
    (out,) = call(
        lambda *refs: last_kernel(n, scale, *refs),
        [(RMAX, n, n, TMAX)],
        [(RMAX, 4 * n, lanes)],
        packed,
        other,
    )
    return out.transpose(0, 3, 1, 2)


def shifted_2(block, axis, distance):
    devices = range(lax.axis_size(axis))
    route = [((i - distance) % len(devices), i) for i in devices]
    return lax.ppermute(block, axis, route)


def plain_times(left_mat, right_mat):
    real_rows = []
    imag_rows = []
    for i in range(3):
        real_cols = []
        imag_cols = []
        for k in range(3):
            real_sum = (
                left_mat[0, i, 0] * right_mat[0, 0, k] - left_mat[1, i, 0] * right_mat[1, 0, k]
            )
            imag_sum = (
                left_mat[0, i, 0] * right_mat[1, 0, k] + left_mat[1, i, 0] * right_mat[0, 0, k]
            )
            for j in range(1, 3):
                real_sum = (
                    real_sum
                    + left_mat[0, i, j] * right_mat[0, j, k]
                    - left_mat[1, i, j] * right_mat[1, j, k]
                )
                imag_sum = (
                    imag_sum
                    + left_mat[0, i, j] * right_mat[1, j, k]
                    + left_mat[1, i, j] * right_mat[0, j, k]
                )
            real_cols.append(real_sum)
            imag_cols.append(imag_sum)
        real_rows.append(jnp.stack(real_cols))
        imag_rows.append(jnp.stack(imag_cols))
    return jnp.stack([jnp.stack(real_rows), jnp.stack(imag_rows)])


def correlation(upper_half, lower_half):
    return jnp.sum(upper_half * lower_half, axis=(0, 1, 2, 5))


def next_x(field, along_dim):
    edge_cells = shifted_2(lax.slice_in_dim(field, 0, 1, axis=along_dim), "gx", -1)
    inner = lax.slice_in_dim(field, 1, field.shape[along_dim], axis=along_dim)
    return jnp.concatenate([inner, edge_cells], axis=along_dim)


def next_t(field):
    edge_cells = shifted_2(lax.slice_in_dim(field, 0, 1, axis=4), "ta", -1)
    inner = lax.slice_in_dim(field, 1, field.shape[4], axis=4)
    return jnp.concatenate([inner, edge_cells], axis=4)


def plain(link_x, link_t):
    all_rows = []
    temporal = [link_t]
    factor = link_t
    for _ in range(1, TMAX):
        factor = next_t(factor)
        temporal.append(plain_times(temporal[-1], factor))
    carried = jnp.stack(temporal)
    spatial = link_x
    factor_x = link_x
    for radius in range(RMAX):
        if radius > 0:
            factor_x = next_x(factor_x, 3)
            spatial = plain_times(spatial, factor_x)
        carried = next_x(carried, 4)
        shifted = spatial
        row_sums = []
        for extent in range(TMAX):
            shifted = next_t(shifted)
            upper_half = plain_times(spatial, carried[extent])
            lower_half = plain_times(temporal[extent], shifted)
            row_sums.append(correlation(upper_half, lower_half))
        all_rows.append(jnp.stack(row_sums))
    local_sums = jnp.stack(all_rows)
    totals = lax.psum(local_sums, "gy")
    return totals / (3.0 * (link_x.shape[5] * lax.axis_size("gy")))


def solution(mesh):
    return jax.shard_map(
        local,
        mesh=mesh,
        in_specs=(P(None, None, None, "gx", "ta", "gy"), P(None, None, None, "gx", "ta", "gy")),
        out_specs=P(None, None, "gx", "ta"),
        check_vma=False,
    )
```
